256 devices in a mesh: seg: 32 (over y_hi, z, core), tp: 8 (over y_lo, x).
Axes of the slice: x: 4, y: 4 (y_hi: 2, y_lo: 2; y = y_hi * 2 + y_lo), z: 8, core: 2. Of those that a mesh axis runs over, the one named last changes fastest.
Arguments:
- tokens: bfloat16 [256, 4096], P('seg'), may hold values from -6 to 6
- w_query: bfloat16 [4096, 4096], P(None, 'tp'), may hold values from -0.09375 to 0.09375
- w_key: bfloat16 [4096, 1024], P(None, 'tp'), may hold values from -0.09375 to 0.09375
- w_value: bfloat16 [4096, 1024], P(None, 'tp'), may hold values from -0.09375 to 0.09375
- w_out: bfloat16 [4096, 4096], P('tp'), may hold values from -0.09375 to 0.09375
- gate_bias: float32 [32], P('tp'), may hold values from -3 to 3
- mem_store: float32 [512, 8, 128, 128], P('seg', 'tp'), may hold values from -6 to 6
- norm_store: float32 [512, 8, 128], P('seg', 'tp'), may hold values from 0.02 to 0.2
- k_cache: bfloat16 [256, 2048, 1024], P('seg', None, 'tp'), may hold values from -2500 to 2500
- v_cache: bfloat16 [256, 2048, 1024], P('seg', None, 'tp'), may hold values from -6 to 6
- home_owner: int32 [256], P('seg'), may hold values from 0 to 31, as said below
- home_slot: int32 [256], P('seg'), may hold values from 0 to 15
- cache_len: int32 [256], P('seg'), may hold values from 1 to 2048
- win_start: int32 [256], P('seg'), may hold values from 0 to 1023
Outputs:
- output: bfloat16 [256, 4096], P('seg', 'tp')
The draws below stay inside these ranges and needn't reach their ends.
Inputs may be any that keep to these rules, and one draw needn't show every extreme that they name: Request b's memory is row 16 * home_owner[b] + home_slot[b] of mem_store and norm_store; no two requests share a row, so one owner holds at most 16 requests, and some owner holds exactly 16.
All inputs are finite; a program needn't handle non-finite values.
Results may differ from the reference program's by a relative error of at most 0.0065.
The reference program's roundings to bfloat16 on the way (of `query`, `key_new`, `value_new`, `memory_read`, `probs` and `attended`) count: a program that leaves them out, or rounds other values in their place, can miss the bound.
Values may be sent and summed in bfloat16 or wider, within the bound.
A program may use at most 128 MiB of HBM per device.

```python
import math
import jax
import jax.numpy as jnp
from jax import lax

D = 4096
H = 32
KVH = 8
DH = 128
WIN = 2048
SLOTS = 16
REQUESTS = 256
N_SEG = 32


def home_pairs(key):
    base_key = jax.random.fold_in(key, 7)
    key_hot, key_bias, key_score, key_order = jax.random.split(base_key, 4)
    slot_total = N_SEG * SLOTS
    global_row = jnp.arange(slot_total, dtype=jnp.int32)
    owner_of = global_row // SLOTS
    hottest = jax.random.randint(key_hot, (), 0, N_SEG)
    owner_bias = jax.random.randint(key_bias, (N_SEG,), 1, 4)
    at_ends = ((owner_of == 0) | (owner_of == N_SEG - 1)) & (global_row % SLOTS == 0)
    row_bias = jnp.where((owner_of == hottest) | at_ends, 0, owner_bias[owner_of])
    random_part = jax.random.randint(key_score, (slot_total,), 0, 65536)
    ranking = (row_bias * 65536 + random_part) * 1024 + global_row
    ordered = jnp.argsort(ranking, stable=True).astype(jnp.int32)
    chosen = ordered[:REQUESTS]
    shuffle = jax.random.permutation(key_order, REQUESTS)
    home_row = jnp.zeros((REQUESTS,), jnp.int32).at[shuffle].set(chosen)
    return ((home_row // SLOTS).astype(jnp.int32), (home_row % SLOTS).astype(jnp.int32))


def draw_home_owner(key, part):
    return home_pairs(key)[0]


def draw_home_slot(key, part):
    return home_pairs(key)[1]


def draw_k_cache(key, part):
    key_base = jax.random.fold_in(jax.random.fold_in(key, 11), 0)
    values = jax.random.normal(key_base, (REQUESTS, WIN, KVH * DH), jnp.float32)
    return values.astype(jnp.bfloat16)


def place_ends(values, rng, smallest, high):
    longest = values.shape.index(max(values.shape))
    spots = []
    for shift in (0, 1):
        where = [jax.random.randint(jax.random.fold_in(rng, axis), (), 0, length) for axis, length in enumerate(values.shape)]
        where[longest] = (where[longest] + shift) % values.shape[longest]
        spots.append(tuple(where))
    return values.at[spots[0]].set(smallest).at[spots[1]].set(high)


def steps_of(rng, dims, shards, smallest, top_value):
    loudness, own = 1.0, jax.random.fold_in(rng, 6)
    for dim, parts in shards:
        draws = jnp.exp(jax.random.uniform(jax.random.fold_in(own, dim), (parts,), jnp.float32, smallest / len(shards), top_value / len(shards)))
        loudness = loudness * jnp.repeat(draws, dims[dim] // parts).reshape([-1 if axis == dim else 1 for axis in range(len(dims))])
    return loudness


def scatter_about(key, extent, width, limit, cuts=(), kind=jnp.bfloat16):
    loudness = steps_of(key, extent, cuts, -0.22, 0.18) if cuts else 1.0
    values = jax.random.normal(key, extent, jnp.float32) * width * loudness
    return jnp.minimum(jnp.maximum(values, -limit), limit).astype(kind)


def setup_inputs(seed: int = 0) -> dict:
    keys = jax.random.split(jax.random.key(seed), 15)
    tokens = scatter_about(keys[0], (REQUESTS, D), 1.0, 6.0, ((0, 32),))
    w_query = scatter_about(keys[1], (D, H * DH), D ** -0.5, 0.09375, ((1, 8),))
    w_key = scatter_about(keys[2], (D, KVH * DH), D ** -0.5, 0.09375, ((1, 8),))
    w_value = scatter_about(keys[3], (D, KVH * DH), D ** -0.5, 0.09375, ((1, 8),))
    w_out = scatter_about(keys[4], (H * DH, D), (H * DH) ** -0.5, 0.09375, ((0, 8),))
    gate_bias = jnp.clip(jax.random.uniform(keys[5], (H,), jnp.float32, -3.0, 3.0) * steps_of(keys[5], (H,), ((0, 8),), -0.4, 0.0), -3.0, 3.0)
    mem_store = scatter_about(keys[6], (N_SEG * SLOTS, KVH, DH, DH), 1.0, 6.0, ((0, 32), (1, 8)), jnp.float32)
    norm_store = jnp.clip(jnp.exp(math.log(0.2) - 2.3025851 * jax.random.uniform(keys[7], (N_SEG * SLOTS, KVH, DH), jnp.float32) ** steps_of(keys[7], (N_SEG * SLOTS, KVH, DH), ((0, 32), (1, 8)), -0.2, 0.2)), 0.02, 0.2)
    k_cache = draw_k_cache(jax.random.fold_in(keys[14], 71), 0)
    v_cache = scatter_about(keys[9], (REQUESTS, WIN, KVH * DH), 1.0, 6.0, ((0, 32), (2, 8)))
    home_owner = draw_home_owner(jax.random.fold_in(keys[14], 71), 0)
    home_slot = draw_home_slot(jax.random.fold_in(keys[14], 71), 0)
    cache_len = place_ends(jax.random.randint(keys[12], (REQUESTS,), 1, WIN + 1), jax.random.fold_in(keys[12], 1), 1, WIN).astype(jnp.int32)
    win_start = place_ends(jax.random.randint(keys[13], (REQUESTS,), 0, WIN // 2), jax.random.fold_in(keys[13], 1), 0, (WIN // 2) - 1).astype(jnp.int32)
    return {"tokens": tokens, "w_query": w_query, "w_key": w_key, "w_value": w_value, "w_out": w_out, "gate_bias": gate_bias, "mem_store": mem_store, "norm_store": norm_store, "k_cache": k_cache, "v_cache": v_cache, "home_owner": home_owner, "home_slot": home_slot, "cache_len": cache_len, "win_start": win_start}


def elu_plus(values):
    return jnp.where(values > 0, values + 1.0, jnp.exp(jnp.minimum(values, 0.0)))


def reference(tokens, w_query, w_key, w_value, w_out, gate_bias, mem_store, norm_store, k_cache, v_cache, home_owner, home_slot, cache_len, win_start):
    group_size = H // KVH
    query = jnp.dot(tokens, w_query, preferred_element_type=jnp.float32).astype(jnp.bfloat16)
    key_new = jnp.dot(tokens, w_key, preferred_element_type=jnp.float32).astype(jnp.bfloat16)
    value_new = jnp.dot(tokens, w_value, preferred_element_type=jnp.float32).astype(jnp.bfloat16)
    query_heads = query.astype(jnp.float32).reshape(REQUESTS, KVH, group_size, DH)
    lifted = elu_plus(query_heads)
    home_row = (home_owner * SLOTS + home_slot).astype(jnp.int32)
    picked = jnp.take(mem_store, home_row, axis=0)
    normed = jnp.take(norm_store, home_row, axis=0)
    numerator = jnp.einsum('bkgi,bkij->bkgj', lifted, picked, precision=lax.Precision.HIGHEST)
    denominator = jnp.einsum('bkgi,bki->bkg', lifted, normed, precision=lax.Precision.HIGHEST)
    memory_read = lax.optimization_barrier((numerator / denominator[..., None]).astype(jnp.bfloat16))
    memory_read = memory_read.astype(jnp.float32)
    score_scale = DH ** -0.5
    cache_keys = k_cache.astype(jnp.float32).reshape(REQUESTS, WIN, KVH, DH)
    cache_values = v_cache.astype(jnp.float32).reshape(REQUESTS, WIN, KVH, DH)
    scores = jnp.einsum('bkgi,bjki->bkgj', query_heads, cache_keys) * score_scale
    own_key = key_new.astype(jnp.float32).reshape(REQUESTS, KVH, DH)
    own_score = jnp.einsum('bkgi,bki->bkg', query_heads, own_key) * score_scale
    position = jnp.arange(WIN, dtype=jnp.int32)
    live_mask = (position[None, :] >= win_start[:, None]) & (position[None, :] < cache_len[:, None])
    live_four = live_mask[:, None, None, :]
    top_score = jnp.maximum(jnp.max(jnp.where(live_four, scores, -jnp.inf), axis=-1), own_score)
    weights = jnp.where(live_four, jnp.exp(scores - top_score[..., None]), 0.0)
    own_weight = jnp.exp(own_score - top_score)
    softmax_total = jnp.sum(weights, axis=-1) + own_weight
    probs = (weights / softmax_total[..., None]).astype(jnp.bfloat16)
    own_prob = (own_weight / softmax_total).astype(jnp.bfloat16)
    local_read = jnp.einsum('bkgj,bjki->bkgi', probs.astype(jnp.float32), cache_values)
    own_value = value_new.astype(jnp.float32).reshape(REQUESTS, KVH, 1, DH)
    local_read = local_read + own_prob.astype(jnp.float32)[..., None] * own_value
    mix_gate = jax.nn.sigmoid(gate_bias).reshape(KVH, group_size)[None, :, :, None]
    attended = (mix_gate * memory_read + (1.0 - mix_gate) * local_read).astype(jnp.bfloat16)
    attended = attended.reshape(REQUESTS, H * DH)
    return jnp.dot(attended, w_out, preferred_element_type=jnp.float32).astype(jnp.bfloat16)
```

```python
import functools

import jax
import jax.numpy as jnp
from jax import lax
from jax.experimental import pallas as pl
from jax.experimental.pallas import tpu as pltpu
from jax.sharding import PartitionSpec as P

DH = 128
GROUP = 4
ROWS = 8
SLOTS = 16
HALF = 2 * DH
TILE = 2 * ROWS

F32 = jnp.float32
BF16 = jnp.bfloat16


def seg_dims(count):
    return {32: (2, 8, 2), 8: (2, 2, 2)}[count]


def tp_dims(count):
    return {8: (2, 4), 2: (2, 1)}[count]


def seg_offsets(dims):
    ny, nz, nc = dims
    found = []
    for dy in range(ny):
        for dz in range(nz):
            for dc in range(nc):
                if (dy, dz, dc) != (0, 0, 0):
                    found.append((-(2 * dy + min(dz, nz - dz)), dc, dy, dz))
    found.sort()
    return [(dy, dz, dc) for _, dc, dy, dz in found]


def tp_offsets(dims):
    ny, nx = dims
    found = []
    for dy in range(ny):
        for dx in range(nx):
            if (dy, dx) != (0, 0):
                found.append((-(dy + min(dx, nx - dx)), dy, dx))
    found.sort()
    return [(dy, dx) for _, dy, dx in found]


def iota(shape, dim):
    return lax.broadcasted_iota(jnp.int32, shape, dim)


def dot(a, b, dims=((1,), (0,))):
    return lax.dot_general(a, b, (dims, ((), ())), preferred_element_type=F32)


def stack_heads(x, rows):
    return jnp.concatenate(
        [x[:rows, :DH], x[:rows, DH:], x[rows:, :DH], x[rows:, DH:]], axis=0
    )


def kernel(
    seg_count,
    tp_count,
    gate_ref,
    owner_ref,
    slot_ref,
    len_ref,
    start_ref,
    tok_h,
    wq_h,
    wk_h,
    wv_h,
    wo_h,
    mem_h,
    norm_h,
    kc_h,
    vc_h,
    out_ref,
    tok,
    wq,
    wkv,
    wo,
    mem,
    norm,
    kc,
    vc,
    mem_hi,
    mem_lo,
    qbuf,
    cbuf,
    sel,
    sel_t,
    rsend,
    rrecv,
    tsend,
    trecv,
    score,
    dsem,
    qs,
    qr,
    cs,
    cr,
    rs,
    rr,
    ts,
    tr,
):
    sdims, tdims = seg_dims(seg_count), tp_dims(tp_count)
    soffs, toffs = seg_offsets(sdims), tp_offsets(tdims)
    me = lax.axis_index("seg")
    my_t = lax.axis_index("tp")
    _, nz, nc = sdims
    my_y, my_z, my_c = me // (nz * nc), (me // nc) % nz, me % nc
    nx = tdims[1]
    my_ty, my_x = my_t // nx, my_t % nx

    def seg_to(off, sign):
        dy, dz, dc = off
        y = (my_y + dy) % sdims[0]
        z = (my_z + sign * dz + nz) % nz
        c = (my_c + dc) % nc
        return (y * nz + z) * nc + c

    def tp_to(off, sign):
        dy, dx = off
        return ((my_ty + dy) % tdims[0]) * nx + (my_x + sign * dx + nx) % nx

    chunks_q, kq = wq.shape[0], wq.shape[1]
    chunks_c, nj = kc.shape[0], kc.shape[2]
    loads = {}
    count = [0]

    def load(name, src, dst):
        loads[name] = pltpu.make_async_copy(src, dst, dsem.at[count[0]])
        count[0] += 1
        loads[name].start()

    load("tok", tok_h, tok)
    for k in range(chunks_q):
        load(f"wq{k}", wq_h.at[pl.ds(k * kq, kq), :], wq.at[k])

    def later():
        load("wk", wk_h, wkv.at[:, pl.ds(0, DH)])
        load("wv", wv_h, wkv.at[:, pl.ds(DH, DH)])
        yield
        load("mem", mem_h, mem)
        load("norm", norm_h, norm)
        yield
        for c in range(chunks_c):
            load(f"k{c}", kc_h.at[:, pl.ds(c * nj, nj), :], kc.at[c])
            yield
        for c in range(chunks_c):
            load(f"v{c}", vc_h.at[:, pl.ds(c * nj, nj), :], vc.at[c])
            yield
        ncol = wo.shape[2]
        for k, off in enumerate(toffs + [(0, 0)]):
            column = pl.multiple_of(tp_to(off, 1) * ncol, ncol)
            load(f"wo{k}", wo_h.at[:, pl.ds(column, ncol)], wo.at[k])
            yield

    pending = later()

    barrier = pltpu.get_barrier_semaphore()
    for off in soffs:
        pl.semaphore_signal(barrier, inc=1, device_id={"seg": seg_to(off, 1)})
    for off in toffs:
        pl.semaphore_signal(barrier, inc=1, device_id={"tp": tp_to(off, 1)})

    lane = iota((1, DH), 1)
    codes = jnp.zeros((1, DH), F32)
    for r in range(ROWS):
        code = (owner_ref[r] * SLOTS + slot_ref[r] - 256).astype(F32)
        codes = jnp.where(lane % ROWS == r, code, codes)
    cbuf[0] = codes

    loads["tok"].wait()
    acc = jnp.zeros((ROWS, GROUP * DH), F32)
    for k in range(chunks_q):
        loads[f"wq{k}"].wait()
        acc = acc + dot(tok[:, pl.ds(k * kq, kq)], wq[k])
        next(pending, None)
    query = acc.astype(BF16).astype(F32)
    qbuf[pl.ds(0, TILE), :] = jnp.concatenate(
        [query[:, :HALF], query[:, HALF:]], axis=0
    ).astype(BF16)
    for _ in pending:
        pass

    pl.semaphore_wait(barrier, len(soffs) + len(toffs))
    code_copies, query_copies = [], []
    for k, off in enumerate(soffs):
        target = {"seg": seg_to(off, 1)}
        copy = pltpu.make_async_remote_copy(
            cbuf.at[0], cbuf.at[k + 1], cs.at[k], cr.at[k], device_id=target
        )
        copy.start()
        code_copies.append(copy)
    for k, off in enumerate(soffs):
        target = {"seg": seg_to(off, 1)}
        copy = pltpu.make_async_remote_copy(
            qbuf.at[pl.ds(0, TILE)],
            qbuf.at[pl.ds((k + 1) * TILE, TILE)],
            qs.at[k],
            qr.at[k],
            device_id=target,
        )
        copy.start()
        query_copies.append(copy)

    loads["mem"].wait()
    loads["norm"].wait()
    flat = mem[...].reshape(SLOTS * DH, DH)
    high = flat.astype(BF16)
    mem_hi[...] = high
    mem_lo[...] = (flat - high.astype(F32)).astype(BF16)

    loads["wk"].wait()
    loads["wv"].wait()
    both = dot(tok[...], wkv[...]).astype(BF16).astype(F32)
    key_new, value_new = both[:, :DH], both[:, DH:]

    nr = GROUP * ROWS
    q32 = jnp.concatenate([query[:, h * DH : (h + 1) * DH] for h in range(GROUP)], axis=0)
    row32 = iota((nr, DH), 0) % ROWS
    scale = DH ** (-0.5)
    own = jnp.sum(q32 * jnp.concatenate([key_new] * GROUP, axis=0), axis=1, keepdims=True)
    own = own * scale

    row1 = iota((nr, 1), 0) % ROWS
    first = jnp.zeros((nr, 1), jnp.int32)
    last = jnp.zeros((nr, 1), jnp.int32)
    for r in range(ROWS):
        first = jnp.where(row1 == r, start_ref[r], first)
        last = jnp.where(row1 == r, len_ref[r], last)

    spread = jnp.concatenate(
        [jnp.where(row32 == r, q32, 0.0) for r in range(ROWS)], axis=1
    ).astype(BF16)
    top = own
    for c in range(chunks_c):
        loads[f"k{c}"].wait()
        keys = jnp.concatenate([kc[c, r] for r in range(ROWS)], axis=1)
        s = dot(spread, keys, ((1,), (1,))) * scale
        position = iota((nr, nj), 1) + c * nj
        s = jnp.where((position >= first) & (position < last), s, -jnp.inf)
        score[c] = s
        top = jnp.maximum(top, jnp.max(s, axis=1, keepdims=True))

    for copy in code_copies:
        copy.wait_recv()
    nmsg = seg_count * TILE
    arrived = cbuf[...].reshape(seg_count, DH).astype(BF16)
    which = (iota((nmsg, seg_count), 0) // TILE == iota((nmsg, seg_count), 1)).astype(F32)
    spread_codes = dot(which.astype(BF16), arrived)
    mrow, mlane = iota((nmsg, DH), 0) % TILE, iota((nmsg, DH), 1)
    code_col = jnp.sum(jnp.where(mrow == mlane, spread_codes, 0.0), axis=1, keepdims=True)
    wanted = (me * SLOTS - 256 + mlane % SLOTS).astype(F32)
    hit = (code_col == wanted) & (mlane // SLOTS == mrow // ROWS)
    picks = jnp.where(hit, 1.0, 0.0)
    sel_t[...] = picks.astype(BF16)
    sel[...] = picks.T[: 2 * SLOTS].astype(BF16)

    own_weight = jnp.exp(own - top)
    total = own_weight
    for c in range(chunks_c):
        w = jnp.exp(score[c] - top)
        score[c] = w
        total = total + jnp.sum(w, axis=1, keepdims=True)
    share = 1.0 / total
    own_prob = (own_weight * share).astype(BF16).astype(F32)

    for copy in query_copies:
        copy.wait_recv()
    lifted = stack_heads(dot(sel[...], qbuf[...]), SLOTS)
    lifted = jnp.where(lifted > 0, lifted + 1.0, jnp.exp(jnp.minimum(lifted, 0.0)))
    norms = jnp.concatenate([norm[...]] * GROUP, axis=0)
    denominator = jnp.sum(lifted * norms, axis=1, keepdims=True)
    nl = GROUP * SLOTS
    slot_row = iota((nl, DH), 0) % SLOTS
    part_hi = lifted.astype(BF16).astype(F32)
    part_lo = lifted - part_hi
    wide_hi = jnp.concatenate(
        [jnp.where(slot_row == t, part_hi, 0.0) for t in range(SLOTS)], axis=1
    ).astype(BF16)
    wide_lo = jnp.concatenate(
        [jnp.where(slot_row == t, part_lo, 0.0) for t in range(SLOTS)], axis=1
    ).astype(BF16)
    stacked = dot(jnp.concatenate([wide_hi, wide_lo], axis=0), mem_hi[...])
    numerator = stacked[:nl] + stacked[nl:] + dot(wide_hi, mem_lo[...])
    read = numerator / denominator
    parts = [read[h * SLOTS : (h + 1) * SLOTS] for h in range(GROUP)]
    read = jnp.concatenate(
        [
            jnp.concatenate(parts[:2], axis=1),
            jnp.concatenate(parts[2:], axis=1),
            jnp.zeros((DH - 2 * SLOTS, HALF), F32),
        ],
        axis=0,
    ).astype(BF16)
    rsend[...] = dot(sel_t[...], read).astype(BF16)
    read_copies = []
    for k, off in enumerate(soffs):
        copy = pltpu.make_async_remote_copy(
            rsend.at[pl.ds((k + 1) * TILE, TILE)],
            rrecv.at[pl.ds(k * TILE, TILE)],
            rs.at[k],
            rr.at[k],
            device_id={"seg": seg_to(off, -1)},
        )
        copy.start()
        read_copies.append(copy)

    wide = jnp.zeros((nr, ROWS * DH), F32)
    for c in range(chunks_c):
        loads[f"v{c}"].wait()
        values = jnp.concatenate([vc[c, r] for r in range(ROWS)], axis=1)
        wide = wide + dot((score[c] * share).astype(BF16), values)
    local = own_prob * jnp.concatenate([value_new] * GROUP, axis=0)
    for r in range(ROWS):
        local = local + jnp.where(row32 == r, wide[:, r * DH : (r + 1) * DH], 0.0)
    gates = jax.nn.sigmoid(
        jnp.concatenate([jnp.full((ROWS, DH), gate_ref[h], F32) for h in range(GROUP)], axis=0)
    )
    local = (1.0 - gates) * local
    for k in range(tp_count):
        loads[f"wo{k}"].wait()

    for copy in read_copies:
        copy.wait_recv()
    back = rsend[pl.ds(0, TILE), :].astype(F32)
    for k in range(len(soffs)):
        back = back + rrecv[pl.ds(k * TILE, TILE), :].astype(F32)
    mixed = gates * stack_heads(back, ROWS) + local
    attended = jnp.concatenate(
        [mixed[h * ROWS : (h + 1) * ROWS] for h in range(GROUP)], axis=1
    ).astype(BF16)

    out_copies = []
    for k, off in enumerate(toffs):
        tsend[k] = dot(attended, wo[k])
        copy = pltpu.make_async_remote_copy(
            tsend.at[k], trecv.at[k], ts.at[k], tr.at[k], device_id={"tp": tp_to(off, 1)}
        )
        copy.start()
        out_copies.append(copy)
    result = dot(attended, wo[tp_count - 1])
    for k, copy in enumerate(out_copies):
        copy.wait_recv()
    for k in range(len(toffs)):
        result = result + trecv[k]
    out_ref[...] = result.astype(BF16)
    for copy in code_copies + query_copies + read_copies + out_copies:
        copy.wait_send()


def body(
    tokens,
    w_query,
    w_key,
    w_value,
    w_out,
    gate_bias,
    mem_store,
    norm_store,
    k_cache,
    v_cache,
    home_owner,
    home_slot,
    cache_len,
    win_start,
):
    seg_count, tp_count = lax.axis_size("seg"), lax.axis_size("tp")
    depth = tokens.shape[1]
    window = k_cache.shape[1]
    width = w_query.shape[1]
    chunks_q, chunks_c = 8, 4
    nj = window // chunks_c
    columns = w_out.shape[1] // tp_count
    peers, partners = seg_count - 1, tp_count - 1
    nmsg = seg_count * TILE
    smem = pl.BlockSpec(memory_space=pltpu.SMEM)
    anywhere = pl.BlockSpec(memory_space=pl.ANY)
    dma = pltpu.SemaphoreType.DMA
    loads = 1 + chunks_q + 4 + 2 * chunks_c + tp_count
    return pl.pallas_call(
        functools.partial(kernel, seg_count, tp_count),
        out_shape=jax.ShapeDtypeStruct((ROWS, columns), BF16),
        in_specs=[smem] * 5 + [anywhere] * 9,
        out_specs=pl.BlockSpec(memory_space=pltpu.VMEM),
        scratch_shapes=[
            pltpu.VMEM((ROWS, depth), BF16),
            pltpu.VMEM((chunks_q, depth // chunks_q, width), BF16),
            pltpu.VMEM((depth, 2 * DH), BF16),
            pltpu.VMEM((tp_count, width, columns), BF16),
            pltpu.VMEM((SLOTS, DH, DH), F32),
            pltpu.VMEM((SLOTS, DH), F32),
            pltpu.VMEM((chunks_c, ROWS, nj, DH), BF16),
            pltpu.VMEM((chunks_c, ROWS, nj, DH), BF16),
            pltpu.VMEM((SLOTS * DH, DH), BF16),
            pltpu.VMEM((SLOTS * DH, DH), BF16),
            pltpu.VMEM((nmsg, HALF), BF16),
            pltpu.VMEM((seg_count, 1, DH), F32),
            pltpu.VMEM((2 * SLOTS, nmsg), BF16),
            pltpu.VMEM((nmsg, DH), BF16),
            pltpu.VMEM((nmsg, HALF), BF16),
            pltpu.VMEM((peers * TILE, HALF), BF16),
            pltpu.VMEM((partners, ROWS, columns), F32),
            pltpu.VMEM((partners, ROWS, columns), F32),
            pltpu.VMEM((chunks_c, GROUP * ROWS, nj), F32),
            dma((loads,)),
            dma((peers,)),
            dma((peers,)),
            dma((peers,)),
            dma((peers,)),
            dma((peers,)),
            dma((peers,)),
            dma((partners,)),
            dma((partners,)),
        ],
        compiler_params=pltpu.CompilerParams(
            collective_id=0, has_side_effects=True, vmem_limit_bytes=60 * 1024 * 1024
        ),
    )(
        gate_bias,
        home_owner,
        home_slot,
        cache_len,
        win_start,
        tokens,
        w_query,
        w_key,
        w_value,
        w_out,
        mem_store.reshape(SLOTS, DH, DH),
        norm_store.reshape(SLOTS, DH),
        k_cache,
        v_cache,
    )


def solution(mesh):
    placed = (
        P("seg", None),
        P(None, "tp"),
        P(None, "tp"),
        P(None, "tp"),
        P("tp", None),
        P("tp"),
        P("seg", "tp", None, None),
        P("seg", "tp", None),
        P("seg", None, "tp"),
        P("seg", None, "tp"),
        P("seg"),
        P("seg"),
        P("seg"),
        P("seg"),
    )
    return jax.shard_map(
        body, mesh=mesh, in_specs=placed, out_specs=P("seg", "tp"), check_vma=False
    )
```

```python
import functools

import jax
import jax.numpy as jnp
from jax import lax
from jax.experimental import pallas as pl
from jax.experimental.pallas import tpu as pltpu
from jax.sharding import PartitionSpec as P

DH = 128
GROUP = 4
ROWS = 8
SLOTS = 16
HALF = 2 * DH
TILE = 2 * ROWS

F32 = jnp.float32
BF16 = jnp.bfloat16


def seg_dims(count):
    return {32: (2, 8, 2), 8: (2, 2, 2)}[count]


def tp_dims(count):
    return {8: (2, 4), 2: (2, 1)}[count]


def seg_offsets(dims):
    ny, nz, _ = dims
    found = []
    for dy in range(ny):
        for dz in range(nz):
            if (dy, dz) != (0, 0):
                found.append((-(2 * dy + min(dz, nz - dz)), dy, dz))
    found.sort()
    return [(dy, dz, 0) for _, dy, dz in found]


def tp_offsets(dims):
    ny, nx = dims
    found = []
    for dy in range(ny):
        for dx in range(nx):
            if (dy, dx) != (0, 0):
                found.append((-(dy + min(dx, nx - dx)), dy, dx))
    found.sort()
    return [(dy, dx) for _, dy, dx in found]


def iota(shape, dim):
    return lax.broadcasted_iota(jnp.int32, shape, dim)


def dot(a, b, dims=((1,), (0,))):
    return lax.dot_general(a, b, (dims, ((), ())), preferred_element_type=F32)


def stack_heads(x, rows):
    return jnp.concatenate(
        [x[:rows, :DH], x[:rows, DH:], x[rows:, :DH], x[rows:, DH:]], axis=0
    )


def stack_halves(x):
    half = x.shape[1] // 2
    return jnp.concatenate([x[:, :half], x[:, half:]], axis=0)


def kernel(
    seg_count,
    tp_count,
    gate_h,
    owner_h,
    slot_h,
    len_h,
    start_h,
    tok_h,
    wq_h,
    wk_h,
    wv_h,
    wo_h,
    mem_h,
    norm_h,
    kc_h,
    vc_h,
    out_ref,
    gate_ref,
    owner_ref,
    slot_ref,
    len_ref,
    start_ref,
    tok,
    wq,
    wkv,
    wo,
    mem,
    norm,
    kc,
    vc,
    mem_hi,
    mem_lo,
    qbuf,
    cbuf,
    sel,
    sel_t,
    xbuf,
    rbuf,
    rsend,
    rrecv,
    tsend,
    trecv,
    score,
    dsem,
    qs,
    qr,
    cs,
    cr,
    rs,
    rr,
    ts,
    tr,
    ps,
    pr,
):
    sdims, tdims = seg_dims(seg_count), tp_dims(tp_count)
    soffs, toffs = seg_offsets(sdims), tp_offsets(tdims)
    me = lax.axis_index("seg")
    my_t = lax.axis_index("tp")
    _, nz, nc = sdims
    my_y, my_z, my_c = me // (nz * nc), (me // nc) % nz, me % nc
    nx = tdims[1]
    my_ty, my_x = my_t // nx, my_t % nx

    def seg_to(off, sign):
        dy, dz, dc = off
        y = (my_y + dy) % sdims[0]
        z = (my_z + sign * dz + nz) % nz
        c = (my_c + dc) % nc
        return (y * nz + z) * nc + c

    def tp_to(off, sign):
        dy, dx = off
        return ((my_ty + dy) % tdims[0]) * nx + (my_x + sign * dx + nx) % nx

    barrier = pltpu.get_barrier_semaphore()
    partner = (0, 0, 1)
    for off in soffs + [partner]:
        pl.semaphore_signal(barrier, inc=1, device_id={"seg": seg_to(off, 1)})
    for off in toffs:
        pl.semaphore_signal(barrier, inc=1, device_id={"tp": tp_to(off, 1)})

    chunks_q, kq = wq.shape[0], wq.shape[1]
    chunks_c, nj = kc.shape[0], kc.shape[2]
    loads = {}
    count = [0]

    def load(name, src, dst):
        loads[name] = pltpu.make_async_copy(src, dst, dsem.at[count[0]])
        count[0] += 1
        loads[name].start()

    load("tok", tok_h, tok)
    load("owner", owner_h, owner_ref)
    load("slot", slot_h, slot_ref)
    for k in range(chunks_q):
        load(f"wq{k}", wq_h.at[pl.ds(k * kq, kq), :], wq.at[k])

    def later():
        load("wk", wk_h, wkv.at[:, pl.ds(0, DH)])
        load("wv", wv_h, wkv.at[:, pl.ds(DH, DH)])
        yield
        load("gate", gate_h, gate_ref)
        load("len", len_h, len_ref)
        load("start", start_h, start_ref)
        load("mem", mem_h, mem)
        load("norm", norm_h, norm)
        yield
        for c in range(chunks_c):
            load(f"k{c}", kc_h.at[:, pl.ds(c * nj, nj), :], kc.at[c])
            yield
        for c in range(chunks_c):
            load(f"v{c}", vc_h.at[:, pl.ds(c * nj, nj), :], vc.at[c])
            yield
        ncol = wo.shape[2]
        for k, off in enumerate(toffs + [(0, 0)]):
            column = pl.multiple_of(tp_to(off, 1) * ncol, ncol)
            load(f"wo{k}", wo_h.at[:, pl.ds(column, ncol)], wo.at[k])
            yield

    pending = later()

    loads["tok"].wait()
    acc = jnp.zeros((ROWS, GROUP * DH), F32)
    for k in range(chunks_q):
        loads[f"wq{k}"].wait()
        acc = acc + dot(tok[:, pl.ds(k * kq, kq)], wq[k])
        next(pending, None)
    query = acc.astype(BF16).astype(F32)
    qbuf[pl.ds(0, TILE), :] = stack_halves(query).astype(BF16)
    for _ in pending:
        pass

    loads["owner"].wait()
    loads["slot"].wait()
    lane = iota((1, DH), 1)
    codes = jnp.zeros((1, DH), F32)
    for r in range(ROWS):
        code = (owner_ref[r] * SLOTS + slot_ref[r] - 256).astype(F32)
        codes = jnp.where(lane % ROWS == r, code, codes)
    cbuf[0] = codes

    pl.semaphore_wait(barrier, len(soffs) + 1 + len(toffs))
    code_copies, query_copies = [], []
    for k, off in enumerate(soffs):
        target = {"seg": seg_to(off, 1)}
        copy = pltpu.make_async_remote_copy(
            cbuf.at[0], cbuf.at[k + 1], cs.at[k], cr.at[k], device_id=target
        )
        copy.start()
        code_copies.append(copy)
    for k, off in enumerate(soffs):
        target = {"seg": seg_to(off, 1)}
        copy = pltpu.make_async_remote_copy(
            qbuf.at[pl.ds(0, TILE)],
            qbuf.at[pl.ds((k + 1) * TILE, TILE)],
            qs.at[k],
            qr.at[k],
            device_id=target,
        )
        copy.start()
        query_copies.append(copy)

    loads["mem"].wait()
    loads["norm"].wait()
    flat = mem[...].reshape(SLOTS * DH, DH)
    high = flat.astype(BF16)
    mem_hi[...] = high
    mem_lo[...] = (flat - high.astype(F32)).astype(BF16)

    loads["wk"].wait()
    loads["wv"].wait()
    both = dot(tok[...], wkv[...]).astype(BF16).astype(F32)
    key_new, value_new = both[:, :DH], both[:, DH:]

    nr = GROUP * ROWS
    q32 = jnp.concatenate([query[:, h * DH : (h + 1) * DH] for h in range(GROUP)], axis=0)
    row32 = iota((nr, DH), 0) % ROWS
    scale = DH ** (-0.5)
    own = jnp.sum(q32 * jnp.concatenate([key_new] * GROUP, axis=0), axis=1, keepdims=True)
    own = own * scale

    for name in ("gate", "len", "start"):
        loads[name].wait()
    row1 = iota((nr, 1), 0) % ROWS
    first = jnp.zeros((nr, 1), jnp.int32)
    last = jnp.zeros((nr, 1), jnp.int32)
    for r in range(ROWS):
        first = jnp.where(row1 == r, start_ref[r], first)
        last = jnp.where(row1 == r, len_ref[r], last)

    rbuf[pl.ds(4 * SLOTS, DH - 4 * SLOTS), :] = jnp.zeros((DH - 4 * SLOTS, HALF), BF16)
    spread = jnp.concatenate(
        [jnp.where(row32 == r, q32, 0.0) for r in range(ROWS)], axis=1
    ).astype(BF16)
    top = own
    for c in range(chunks_c):
        loads[f"k{c}"].wait()
        keys = jnp.concatenate([kc[c, r] for r in range(ROWS)], axis=1)
        s = dot(spread, keys, ((1,), (1,))) * scale
        position = iota((nr, nj), 1) + c * nj
        s = jnp.where((position >= first) & (position < last), s, -jnp.inf)
        score[c] = s
        top = jnp.maximum(top, jnp.max(s, axis=1, keepdims=True))

    for copy in code_copies:
        copy.wait_recv()
    senders = cbuf.shape[0]
    nmsg = senders * TILE
    arrived = cbuf[...].reshape(senders, DH).astype(BF16)
    which = (iota((nmsg, senders), 0) // TILE == iota((nmsg, senders), 1)).astype(F32)
    spread_codes = dot(which.astype(BF16), arrived)
    mrow, mlane = iota((nmsg, DH), 0) % TILE, iota((nmsg, DH), 1)
    code_col = jnp.sum(jnp.where(mrow == mlane, spread_codes, 0.0), axis=1, keepdims=True)
    holder = jnp.where(mlane < 2 * SLOTS, me, seg_to(partner, 1))
    wanted = (holder * SLOTS - 256 + mlane % SLOTS).astype(F32)
    hit = (code_col == wanted) & ((mlane // SLOTS) % 2 == mrow // ROWS) & (mlane < 4 * SLOTS)
    picks = jnp.where(hit, 1.0, 0.0)
    sel_t[...] = picks.astype(BF16)
    sel[...] = picks.T[: 4 * SLOTS].astype(BF16)

    own_weight = jnp.exp(own - top)
    total = own_weight
    for c in range(chunks_c):
        w = jnp.exp(score[c] - top)
        score[c] = w
        total = total + jnp.sum(w, axis=1, keepdims=True)
    share = 1.0 / total
    own_prob = (own_weight * share).astype(BF16).astype(F32)

    for copy in query_copies:
        copy.wait_recv()
    picked = dot(sel[...], qbuf[...])
    own_half, other_half = pl.ds(0, 2 * SLOTS), pl.ds(2 * SLOTS, 2 * SLOTS)
    xbuf[own_half, :] = picked[2 * SLOTS :].astype(BF16)
    other = {"seg": seg_to(partner, 1)}
    pick_copy = pltpu.make_async_remote_copy(
        xbuf.at[own_half], xbuf.at[other_half], ps.at[0], pr.at[0], device_id=other
    )
    pick_copy.start()
    pick_copy.wait_recv()
    picked = picked[: 2 * SLOTS] + xbuf[other_half, :].astype(F32)
    lifted = stack_heads(picked, SLOTS)
    lifted = jnp.where(lifted > 0, lifted + 1.0, jnp.exp(jnp.minimum(lifted, 0.0)))
    norms = jnp.concatenate([norm[...]] * GROUP, axis=0)
    denominator = jnp.sum(lifted * norms, axis=1, keepdims=True)
    nl = GROUP * SLOTS
    slot_row = iota((nl, DH), 0) % SLOTS
    part_hi = lifted.astype(BF16).astype(F32)
    part_lo = lifted - part_hi
    wide_hi = jnp.concatenate(
        [jnp.where(slot_row == t, part_hi, 0.0) for t in range(SLOTS)], axis=1
    ).astype(BF16)
    wide_lo = jnp.concatenate(
        [jnp.where(slot_row == t, part_lo, 0.0) for t in range(SLOTS)], axis=1
    ).astype(BF16)
    stacked = dot(jnp.concatenate([wide_hi, wide_lo], axis=0), mem_hi[...])
    numerator = stacked[:nl] + stacked[nl:] + dot(wide_hi, mem_lo[...])
    read = numerator / denominator
    parts = [read[h * SLOTS : (h + 1) * SLOTS] for h in range(GROUP)]
    rbuf[own_half, :] = jnp.concatenate(
        [jnp.concatenate(parts[:2], axis=1), jnp.concatenate(parts[2:], axis=1)], axis=0
    ).astype(BF16)
    swap_copy = pltpu.make_async_remote_copy(
        rbuf.at[own_half], rbuf.at[other_half], ps.at[1], pr.at[1], device_id=other
    )
    swap_copy.start()
    swap_copy.wait_recv()
    rsend[...] = dot(sel_t[...], rbuf[...]).astype(BF16)
    read_copies = []
    for k, off in enumerate(soffs):
        copy = pltpu.make_async_remote_copy(
            rsend.at[pl.ds((k + 1) * TILE, TILE)],
            rrecv.at[pl.ds(k * TILE, TILE)],
            rs.at[k],
            rr.at[k],
            device_id={"seg": seg_to(off, -1)},
        )
        copy.start()
        read_copies.append(copy)

    wide = jnp.zeros((nr, ROWS * DH), F32)
    for c in range(chunks_c):
        loads[f"v{c}"].wait()
        values = jnp.concatenate([vc[c, r] for r in range(ROWS)], axis=1)
        wide = wide + dot((score[c] * share).astype(BF16), values)
    local = own_prob * jnp.concatenate([value_new] * GROUP, axis=0)
    for r in range(ROWS):
        local = local + jnp.where(row32 == r, wide[:, r * DH : (r + 1) * DH], 0.0)
    gates = jax.nn.sigmoid(
        jnp.concatenate([jnp.full((ROWS, DH), gate_ref[h], F32) for h in range(GROUP)], axis=0)
    )
    local = (1.0 - gates) * local
    for k in range(tp_count):
        loads[f"wo{k}"].wait()

    for copy in read_copies:
        copy.wait_recv()
    back = rsend[pl.ds(0, TILE), :].astype(F32)
    for k in range(len(soffs)):
        back = back + rrecv[pl.ds(k * TILE, TILE), :].astype(F32)
    mixed = gates * stack_heads(back, ROWS) + local
    attended = jnp.concatenate(
        [mixed[h * ROWS : (h + 1) * ROWS] for h in range(GROUP)], axis=1
    ).astype(BF16)

    out_copies = []
    for k, off in enumerate(toffs):
        tsend[k] = stack_halves(dot(attended, wo[k])).astype(BF16)
        copy = pltpu.make_async_remote_copy(
            tsend.at[k], trecv.at[k], ts.at[k], tr.at[k], device_id={"tp": tp_to(off, 1)}
        )
        copy.start()
        out_copies.append(copy)
    result = stack_halves(dot(attended, wo[tp_count - 1]))
    for k, copy in enumerate(out_copies):
        copy.wait_recv()
    for k in range(len(toffs)):
        result = result + trecv[k].astype(F32)
    out_ref[...] = jnp.concatenate([result[:ROWS], result[ROWS:]], axis=1).astype(BF16)
    for copy in code_copies + query_copies + read_copies + out_copies + [pick_copy, swap_copy]:
        copy.wait_send()


def body(
    tokens,
    w_query,
    w_key,
    w_value,
    w_out,
    gate_bias,
    mem_store,
    norm_store,
    k_cache,
    v_cache,
    home_owner,
    home_slot,
    cache_len,
    win_start,
):
    seg_count, tp_count = lax.axis_size("seg"), lax.axis_size("tp")
    depth = tokens.shape[1]
    window = k_cache.shape[1]
    width = w_query.shape[1]
    chunks_q, chunks_c = 8, 4
    nj = window // chunks_c
    columns = w_out.shape[1] // tp_count
    senders = seg_count // seg_dims(seg_count)[2]
    peers, partners = senders - 1, tp_count - 1
    nmsg = senders * TILE
    anywhere = pl.BlockSpec(memory_space=pl.ANY)
    dma = pltpu.SemaphoreType.DMA
    loads = 1 + chunks_q + 9 + 2 * chunks_c + tp_count
    return pl.pallas_call(
        functools.partial(kernel, seg_count, tp_count),
        out_shape=jax.ShapeDtypeStruct((ROWS, columns), BF16),
        in_specs=[anywhere] * 14,
        out_specs=pl.BlockSpec(memory_space=pltpu.VMEM),
        scratch_shapes=[
            pltpu.SMEM((GROUP,), F32),
            pltpu.SMEM((ROWS,), jnp.int32),
            pltpu.SMEM((ROWS,), jnp.int32),
            pltpu.SMEM((ROWS,), jnp.int32),
            pltpu.SMEM((ROWS,), jnp.int32),
            pltpu.VMEM((ROWS, depth), BF16),
            pltpu.VMEM((chunks_q, depth // chunks_q, width), BF16),
            pltpu.VMEM((depth, 2 * DH), BF16),
            pltpu.VMEM((tp_count, width, columns), BF16),
            pltpu.VMEM((SLOTS, DH, DH), F32),
            pltpu.VMEM((SLOTS, DH), F32),
            pltpu.VMEM((chunks_c, ROWS, nj, DH), BF16),
            pltpu.VMEM((chunks_c, ROWS, nj, DH), BF16),
            pltpu.VMEM((SLOTS * DH, DH), BF16),
            pltpu.VMEM((SLOTS * DH, DH), BF16),
            pltpu.VMEM((nmsg, HALF), BF16),
            pltpu.VMEM((senders, 1, DH), F32),
            pltpu.VMEM((4 * SLOTS, nmsg), BF16),
            pltpu.VMEM((nmsg, DH), BF16),
            pltpu.VMEM((4 * SLOTS, HALF), BF16),
            pltpu.VMEM((DH, HALF), BF16),
            pltpu.VMEM((nmsg, HALF), BF16),
            pltpu.VMEM((peers * TILE, HALF), BF16),
            pltpu.VMEM((partners, 2 * ROWS, columns // 2), BF16),
            pltpu.VMEM((partners, 2 * ROWS, columns // 2), BF16),
            pltpu.VMEM((chunks_c, GROUP * ROWS, nj), F32),
            dma((loads,)),
            dma((peers,)),
            dma((peers,)),
            dma((peers,)),
            dma((peers,)),
            dma((peers,)),
            dma((peers,)),
            dma((partners,)),
            dma((partners,)),
            dma((2,)),
            dma((2,)),
        ],
        compiler_params=pltpu.CompilerParams(
            collective_id=0, has_side_effects=True, vmem_limit_bytes=60 * 1024 * 1024
        ),
    )(
        gate_bias,
        home_owner,
        home_slot,
        cache_len,
        win_start,
        tokens,
        w_query,
        w_key,
        w_value,
        w_out,
        mem_store.reshape(SLOTS, DH, DH),
        norm_store.reshape(SLOTS, DH),
        k_cache,
        v_cache,
    )


def solution(mesh):
    placed = (
        P("seg", None),
        P(None, "tp"),
        P(None, "tp"),
        P(None, "tp"),
        P("tp", None),
        P("tp"),
        P("seg", "tp", None, None),
        P("seg", "tp", None),
        P("seg", None, "tp"),
        P("seg", None, "tp"),
        P("seg"),
        P("seg"),
        P("seg"),
        P("seg"),
    )
    return jax.shard_map(
        body, mesh=mesh, in_specs=placed, out_specs=P("seg", "tp"), check_vma=False
    )
```

```python
import functools

import jax
import jax.numpy as jnp
from jax import lax
from jax.experimental import pallas as pl
from jax.experimental.pallas import tpu as pltpu
from jax.sharding import PartitionSpec as P

DH = 128
GROUP = 4
ROWS = 8
SLOTS = 16
HALF = 2 * DH
TILE = 2 * ROWS

F32 = jnp.float32
BF16 = jnp.bfloat16


def seg_dims(count):
    return {32: (2, 8, 2), 8: (2, 2, 2)}[count]


def tp_dims(count):
    return {8: (2, 4), 2: (2, 1)}[count]


def seg_offsets(dims):
    ny, nz, _ = dims
    found = []
    for dy in range(ny):
        for dz in range(nz):
            if (dy, dz) != (0, 0):
                found.append((-(2 * dy + min(dz, nz - dz)), dy, dz))
    found.sort()
    return [(dy, dz, 0) for _, dy, dz in found]


def tp_offsets(dims):
    ny, nx = dims
    found = []
    for dy in range(ny):
        for dx in range(nx):
            if (dy, dx) != (0, 0):
                found.append((-(dy + min(dx, nx - dx)), dy, dx))
    found.sort()
    return [(dy, dx) for _, dy, dx in found]


def iota(shape, dim):
    return lax.broadcasted_iota(jnp.int32, shape, dim)


def dot(a, b, dims=((1,), (0,))):
    return lax.dot_general(a, b, (dims, ((), ())), preferred_element_type=F32)


def stack_heads(x, rows):
    return jnp.concatenate(
        [x[:rows, :DH], x[:rows, DH:], x[rows:, :DH], x[rows:, DH:]], axis=0
    )


def stack_halves(x):
    half = x.shape[1] // 2
    return jnp.concatenate([x[:, :half], x[:, half:]], axis=0)


def kernel(
    seg_count,
    tp_count,
    gate_h,
    owner_h,
    slot_h,
    len_h,
    start_h,
    tok_h,
    wq_h,
    wk_h,
    wv_h,
    wo_h,
    mem_h,
    norm_h,
    kc_h,
    vc_h,
    out_ref,
    gate_ref,
    owner_ref,
    slot_ref,
    len_ref,
    start_ref,
    tok,
    wq,
    wkv,
    wo,
    mem,
    norm,
    kc,
    vc,
    mem_hi,
    mem_lo,
    qbuf,
    cbuf,
    sel,
    sel_t,
    xbuf,
    rbuf,
    rsend,
    rrecv,
    tsend,
    trecv,
    score,
    dsem,
    qs,
    qr,
    cs,
    cr,
    rs,
    rr,
    ts,
    tr,
    ps,
    pr,
):
    sdims, tdims = seg_dims(seg_count), tp_dims(tp_count)
    soffs, toffs = seg_offsets(sdims), tp_offsets(tdims)
    me = lax.axis_index("seg")
    my_t = lax.axis_index("tp")
    _, nz, nc = sdims
    my_y, my_z, my_c = me // (nz * nc), (me // nc) % nz, me % nc
    nx = tdims[1]
    my_ty, my_x = my_t // nx, my_t % nx

    def seg_to(off, sign):
        dy, dz, dc = off
        y = (my_y + dy) % sdims[0]
        z = (my_z + sign * dz + nz) % nz
        c = (my_c + dc) % nc
        return (y * nz + z) * nc + c

    def tp_to(off, sign):
        dy, dx = off
        return ((my_ty + dy) % tdims[0]) * nx + (my_x + sign * dx + nx) % nx

    barrier = pltpu.get_barrier_semaphore()
    partner = (0, 0, 1)
    for off in soffs + [partner]:
        pl.semaphore_signal(barrier, inc=1, device_id={"seg": seg_to(off, 1)})
    for off in toffs:
        pl.semaphore_signal(barrier, inc=1, device_id={"tp": tp_to(off, 1)})

    chunks_q, kq = wq.shape[0], wq.shape[1]
    chunks_c, nj = kc.shape[0], kc.shape[2]
    loads = {}
    count = [0]

    def load(name, src, dst):
        loads[name] = pltpu.make_async_copy(src, dst, dsem.at[count[0]])
        count[0] += 1
        loads[name].start()

    load("tok", tok_h, tok)
    load("owner", owner_h, owner_ref)
    load("slot", slot_h, slot_ref)
    for k in range(chunks_q):
        load(f"wq{k}", wq_h.at[pl.ds(k * kq, kq), :], wq.at[k])

    def later():
        load("wk", wk_h, wkv.at[:, pl.ds(0, DH)])
        load("wv", wv_h, wkv.at[:, pl.ds(DH, DH)])
        yield
        load("gate", gate_h, gate_ref)
        load("len", len_h, len_ref)
        load("start", start_h, start_ref)
        load("mem", mem_h, mem)
        load("norm", norm_h, norm)
        yield
        for c in range(chunks_c):
            load(f"k{c}", kc_h.at[:, pl.ds(c * nj, nj), :], kc.at[c])
            yield
        for c in range(chunks_c):
            load(f"v{c}", vc_h.at[:, pl.ds(c * nj, nj), :], vc.at[c])
            yield
        ncol = wo.shape[2]
        for k, off in enumerate(toffs + [(0, 0)]):
            column = pl.multiple_of(tp_to(off, 1) * ncol, ncol)
            load(f"wo{k}", wo_h.at[:, pl.ds(column, ncol)], wo.at[k])
            yield

    pending = later()

    loads["tok"].wait()
    acc = jnp.zeros((ROWS, GROUP * DH), F32)
    for k in range(chunks_q):
        loads[f"wq{k}"].wait()
        acc = acc + dot(tok[:, pl.ds(k * kq, kq)], wq[k])
        next(pending, None)
    query = acc.astype(BF16).astype(F32)
    qbuf[pl.ds(0, TILE), :] = stack_halves(query).astype(BF16)
    for _ in pending:
        pass

    loads["owner"].wait()
    loads["slot"].wait()
    lane = iota((1, DH), 1)
    codes = jnp.zeros((1, DH), F32)
    for r in range(ROWS):
        code = (owner_ref[r] * SLOTS + slot_ref[r] - 256).astype(F32)
        codes = jnp.where(lane % ROWS == r, code, codes)
    cbuf[0] = codes

    pl.semaphore_wait(barrier, len(soffs) + 1 + len(toffs))
    code_copies, query_copies = [], []
    for k, off in enumerate(soffs):
        target = {"seg": seg_to(off, 1)}
        copy = pltpu.make_async_remote_copy(
            cbuf.at[0], cbuf.at[k + 1], cs.at[k], cr.at[k], device_id=target
        )
        copy.start()
        code_copies.append(copy)
    for k, off in enumerate(soffs):
        target = {"seg": seg_to(off, 1)}
        copy = pltpu.make_async_remote_copy(
            qbuf.at[pl.ds(0, TILE)],
            qbuf.at[pl.ds((k + 1) * TILE, TILE)],
            qs.at[k],
            qr.at[k],
            device_id=target,
        )
        copy.start()
        query_copies.append(copy)

    loads["mem"].wait()
    loads["norm"].wait()
    flat = mem[...].reshape(SLOTS * DH, DH)
    high = flat.astype(BF16)
    mem_hi[...] = high
    mem_lo[...] = (flat - high.astype(F32)).astype(BF16)

    loads["wk"].wait()
    loads["wv"].wait()
    both = dot(tok[...], wkv[...]).astype(BF16).astype(F32)
    key_new, value_new = both[:, :DH], both[:, DH:]

    nr = GROUP * ROWS
    q32 = jnp.concatenate([query[:, h * DH : (h + 1) * DH] for h in range(GROUP)], axis=0)
    row32 = iota((nr, DH), 0) % ROWS
    scale = DH ** (-0.5)
    own = jnp.sum(q32 * jnp.concatenate([key_new] * GROUP, axis=0), axis=1, keepdims=True)
    own = own * scale

    for name in ("gate", "len", "start"):
        loads[name].wait()
    row1 = iota((nr, 1), 0) % ROWS
    first = jnp.zeros((nr, 1), jnp.int32)
    last = jnp.zeros((nr, 1), jnp.int32)
    for r in range(ROWS):
        first = jnp.where(row1 == r, start_ref[r], first)
        last = jnp.where(row1 == r, len_ref[r], last)

    rbuf[pl.ds(4 * SLOTS, DH - 4 * SLOTS), :] = jnp.zeros((DH - 4 * SLOTS, HALF), BF16)
    spread = jnp.concatenate(
        [jnp.where(row32 == r, q32, 0.0) for r in range(ROWS)], axis=1
    ).astype(BF16)
    top = own
    for c in range(chunks_c):
        loads[f"k{c}"].wait()
        keys = jnp.concatenate([kc[c, r] for r in range(ROWS)], axis=1)
        s = dot(spread, keys, ((1,), (1,))) * scale
        position = iota((nr, nj), 1) + c * nj
        s = jnp.where((position >= first) & (position < last), s, -jnp.inf)
        score[c] = s
        top = jnp.maximum(top, jnp.max(s, axis=1, keepdims=True))

    for copy in code_copies:
        copy.wait_recv()
    senders = cbuf.shape[0]
    nmsg = senders * TILE
    arrived = cbuf[...].reshape(senders, DH).astype(BF16)
    which = (iota((nmsg, senders), 0) // TILE == iota((nmsg, senders), 1)).astype(F32)
    spread_codes = dot(which.astype(BF16), arrived)
    mrow, mlane = iota((nmsg, DH), 0) % TILE, iota((nmsg, DH), 1)
    code_col = jnp.sum(jnp.where(mrow == mlane, spread_codes, 0.0), axis=1, keepdims=True)
    holder = jnp.where(mlane < 2 * SLOTS, me, seg_to(partner, 1))
    wanted = (holder * SLOTS - 256 + mlane % SLOTS).astype(F32)
    hit = (code_col == wanted) & ((mlane // SLOTS) % 2 == mrow // ROWS) & (mlane < 4 * SLOTS)
    picks = jnp.where(hit, 1.0, 0.0)
    sel_t[...] = picks.astype(BF16)
    sel[...] = picks.T[: 4 * SLOTS].astype(BF16)

    own_weight = jnp.exp(own - top)
    total = own_weight
    for c in range(chunks_c):
        w = jnp.exp(score[c] - top)
        score[c] = w
        total = total + jnp.sum(w, axis=1, keepdims=True)
    share = 1.0 / total
    own_prob = (own_weight * share).astype(BF16).astype(F32)

    for copy in query_copies:
        copy.wait_recv()
    picked = dot(sel[...], qbuf[...])
    own_half, other_half = pl.ds(0, 2 * SLOTS), pl.ds(2 * SLOTS, 2 * SLOTS)
    xbuf[own_half, :] = picked[2 * SLOTS :].astype(BF16)
    other = {"seg": seg_to(partner, 1)}
    pick_copy = pltpu.make_async_remote_copy(
        xbuf.at[own_half], xbuf.at[other_half], ps.at[0], pr.at[0], device_id=other
    )
    pick_copy.start()
    pick_copy.wait_recv()
    picked = picked[: 2 * SLOTS] + xbuf[other_half, :].astype(F32)
    lifted = stack_heads(picked, SLOTS)
    lifted = jnp.where(lifted > 0, lifted + 1.0, jnp.exp(jnp.minimum(lifted, 0.0)))
    norms = jnp.concatenate([norm[...]] * GROUP, axis=0)
    denominator = jnp.sum(lifted * norms, axis=1, keepdims=True)
    nl = GROUP * SLOTS
    slot_row = iota((nl, DH), 0) % SLOTS
    part_hi = lifted.astype(BF16).astype(F32)
    part_lo = lifted - part_hi
    wide_hi = jnp.concatenate(
        [jnp.where(slot_row == t, part_hi, 0.0) for t in range(SLOTS)], axis=1
    ).astype(BF16)
    wide_lo = jnp.concatenate(
        [jnp.where(slot_row == t, part_lo, 0.0) for t in range(SLOTS)], axis=1
    ).astype(BF16)
    stacked = dot(jnp.concatenate([wide_hi, wide_lo], axis=0), mem_hi[...])
    numerator = stacked[:nl] + stacked[nl:] + dot(wide_hi, mem_lo[...])
    read = numerator / denominator
    parts = [read[h * SLOTS : (h + 1) * SLOTS] for h in range(GROUP)]
    rbuf[own_half, :] = jnp.concatenate(
        [jnp.concatenate(parts[:2], axis=1), jnp.concatenate(parts[2:], axis=1)], axis=0
    ).astype(BF16)
    swap_copy = pltpu.make_async_remote_copy(
        rbuf.at[own_half], rbuf.at[other_half], ps.at[1], pr.at[1], device_id=other
    )
    swap_copy.start()
    swap_copy.wait_recv()
    rsend[...] = dot(sel_t[...], rbuf[...]).astype(BF16)
    read_copies = []
    for k, off in enumerate(soffs):
        copy = pltpu.make_async_remote_copy(
            rsend.at[pl.ds((k + 1) * TILE, TILE)],
            rrecv.at[pl.ds(k * TILE, TILE)],
            rs.at[k],
            rr.at[k],
            device_id={"seg": seg_to(off, -1)},
        )
        copy.start()
        read_copies.append(copy)

    wide = jnp.zeros((nr, ROWS * DH), F32)
    for c in range(chunks_c):
        loads[f"v{c}"].wait()
        values = jnp.concatenate([vc[c, r] for r in range(ROWS)], axis=1)
        wide = wide + dot((score[c] * share).astype(BF16), values)
    local = own_prob * jnp.concatenate([value_new] * GROUP, axis=0)
    for r in range(ROWS):
        local = local + jnp.where(row32 == r, wide[:, r * DH : (r + 1) * DH], 0.0)
    gates = jax.nn.sigmoid(
        jnp.concatenate([jnp.full((ROWS, DH), gate_ref[h], F32) for h in range(GROUP)], axis=0)
    )
    local = (1.0 - gates) * local
    for k in range(tp_count):
        loads[f"wo{k}"].wait()

    for copy in read_copies:
        copy.wait_recv()
    back = rsend[pl.ds(0, TILE), :].astype(F32)
    for k in range(len(soffs)):
        back = back + rrecv[pl.ds(k * TILE, TILE), :].astype(F32)
    mixed = gates * stack_heads(back, ROWS) + local
    attended = jnp.concatenate(
        [mixed[h * ROWS : (h + 1) * ROWS] for h in range(GROUP)], axis=1
    ).astype(BF16)

    out_copies = []
    for k, off in enumerate(toffs):
        tsend[k] = stack_halves(dot(attended, wo[k])).astype(BF16)
        copy = pltpu.make_async_remote_copy(
            tsend.at[k], trecv.at[k], ts.at[k], tr.at[k], device_id={"tp": tp_to(off, 1)}
        )
        copy.start()
        out_copies.append(copy)
    result = stack_halves(dot(attended, wo[tp_count - 1]))
    for k, copy in enumerate(out_copies):
        copy.wait_recv()
    for k in range(len(toffs)):
        result = result + trecv[k].astype(F32)
    out_ref[...] = jnp.concatenate([result[:ROWS], result[ROWS:]], axis=1).astype(BF16)
    for copy in code_copies + query_copies + read_copies + out_copies + [pick_copy, swap_copy]:
        copy.wait_send()


def body(
    tokens,
    w_query,
    w_key,
    w_value,
    w_out,
    gate_bias,
    mem_store,
    norm_store,
    k_cache,
    v_cache,
    home_owner,
    home_slot,
    cache_len,
    win_start,
):
    seg_count, tp_count = lax.axis_size("seg"), lax.axis_size("tp")
    depth = tokens.shape[1]
    window = k_cache.shape[1]
    width = w_query.shape[1]
    chunks_q, chunks_c = 8, 4
    nj = window // chunks_c
    columns = w_out.shape[1] // tp_count
    senders = seg_count // seg_dims(seg_count)[2]
    peers, partners = senders - 1, tp_count - 1
    nmsg = senders * TILE
    anywhere = pl.BlockSpec(memory_space=pl.ANY)
    dma = pltpu.SemaphoreType.DMA
    loads = 1 + chunks_q + 9 + 2 * chunks_c + tp_count
    return pl.pallas_call(
        functools.partial(kernel, seg_count, tp_count),
        out_shape=pltpu.VMEM((ROWS, columns), BF16),
        in_specs=[anywhere] * 14,
        out_specs=pl.BlockSpec(memory_space=pltpu.VMEM),
        scratch_shapes=[
            pltpu.SMEM((GROUP,), F32),
            pltpu.SMEM((ROWS,), jnp.int32),
            pltpu.SMEM((ROWS,), jnp.int32),
            pltpu.SMEM((ROWS,), jnp.int32),
            pltpu.SMEM((ROWS,), jnp.int32),
            pltpu.VMEM((ROWS, depth), BF16),
            pltpu.VMEM((chunks_q, depth // chunks_q, width), BF16),
            pltpu.VMEM((depth, 2 * DH), BF16),
            pltpu.VMEM((tp_count, width, columns), BF16),
            pltpu.VMEM((SLOTS, DH, DH), F32),
            pltpu.VMEM((SLOTS, DH), F32),
            pltpu.VMEM((chunks_c, ROWS, nj, DH), BF16),
            pltpu.VMEM((chunks_c, ROWS, nj, DH), BF16),
            pltpu.VMEM((SLOTS * DH, DH), BF16),
            pltpu.VMEM((SLOTS * DH, DH), BF16),
            pltpu.VMEM((nmsg, HALF), BF16),
            pltpu.VMEM((senders, 1, DH), F32),
            pltpu.VMEM((4 * SLOTS, nmsg), BF16),
            pltpu.VMEM((nmsg, DH), BF16),
            pltpu.VMEM((4 * SLOTS, HALF), BF16),
            pltpu.VMEM((DH, HALF), BF16),
            pltpu.VMEM((nmsg, HALF), BF16),
            pltpu.VMEM((peers * TILE, HALF), BF16),
            pltpu.VMEM((partners, 2 * ROWS, columns // 2), BF16),
            pltpu.VMEM((partners, 2 * ROWS, columns // 2), BF16),
            pltpu.VMEM((chunks_c, GROUP * ROWS, nj), F32),
            dma((loads,)),
            dma((peers,)),
            dma((peers,)),
            dma((peers,)),
            dma((peers,)),
            dma((peers,)),
            dma((peers,)),
            dma((partners,)),
            dma((partners,)),
            dma((2,)),
            dma((2,)),
        ],
        compiler_params=pltpu.CompilerParams(
            collective_id=0, has_side_effects=True, vmem_limit_bytes=60 * 1024 * 1024
        ),
    )(
        gate_bias,
        home_owner,
        home_slot,
        cache_len,
        win_start,
        tokens,
        w_query,
        w_key,
        w_value,
        w_out,
        mem_store.reshape(SLOTS, DH, DH),
        norm_store.reshape(SLOTS, DH),
        k_cache,
        v_cache,
    )


def solution(mesh):
    placed = (
        P("seg", None),
        P(None, "tp"),
        P(None, "tp"),
        P(None, "tp"),
        P("tp", None),
        P("tp"),
        P("seg", "tp", None, None),
        P("seg", "tp", None),
        P("seg", None, "tp"),
        P("seg", None, "tp"),
        P("seg"),
        P("seg"),
        P("seg"),
        P("seg"),
    )
    return jax.shard_map(
        body, mesh=mesh, in_specs=placed, out_specs=P("seg", "tp"), check_vma=False
    )
```

```python
import functools

import jax
import jax.numpy as jnp
from jax import lax
from jax.experimental import pallas as pl
from jax.experimental.pallas import tpu as pltpu
from jax.sharding import PartitionSpec as P

DH = 128
GROUP = 4
ROWS = 8
SLOTS = 16
HALF = 2 * DH
TILE = 2 * ROWS

F32 = jnp.float32
BF16 = jnp.bfloat16


def seg_dims(count):
    return {32: (2, 8, 2), 8: (2, 2, 2)}[count]


def tp_dims(count):
    return {8: (2, 4), 2: (2, 1)}[count]


def seg_offsets(dims):
    ny, nz, _ = dims
    found = []
    for dy in range(ny):
        for dz in range(nz):
            if (dy, dz) != (0, 0):
                found.append((-(2 * dy + min(dz, nz - dz)), dy, dz))
    found.sort()
    return [(dy, dz, 0) for _, dy, dz in found]


def tp_offsets(dims):
    ny, nx = dims
    found = []
    for dy in range(ny):
        for dx in range(nx):
            if (dy, dx) != (0, 0):
                found.append((-(dy + min(dx, nx - dx)), dy, dx))
    found.sort()
    return [(dy, dx) for _, dy, dx in found]


def iota(shape, dim):
    return lax.broadcasted_iota(jnp.int32, shape, dim)


def dot(a, b, dims=((1,), (0,))):
    return lax.dot_general(a, b, (dims, ((), ())), preferred_element_type=F32)


def stack_heads(x, rows):
    return jnp.concatenate(
        [x[:rows, :DH], x[:rows, DH:], x[rows:, :DH], x[rows:, DH:]], axis=0
    )


def stack_halves(x):
    half = x.shape[1] // 2
    return jnp.concatenate([x[:, :half], x[:, half:]], axis=0)


def kernel(
    seg_count,
    tp_count,
    gate_h,
    owner_h,
    slot_h,
    len_h,
    start_h,
    tok_h,
    wq_h,
    wk_h,
    wv_h,
    wo_h,
    mem_h,
    norm_h,
    kc_h,
    vc_h,
    out_ref,
    gate_ref,
    owner_ref,
    slot_ref,
    len_ref,
    start_ref,
    tok,
    wq,
    wkv,
    wo,
    mem,
    norm,
    kc,
    vc,
    mem_hi,
    mem_lo,
    qbuf,
    cbuf,
    sel,
    sel_t,
    xbuf,
    rbuf,
    rsend,
    rrecv,
    tsend,
    trecv,
    score,
    dsem,
    qs,
    qr,
    cs,
    cr,
    rs,
    rr,
    ts,
    tr,
    ps,
    pr,
):
    sdims, tdims = seg_dims(seg_count), tp_dims(tp_count)
    soffs, toffs = seg_offsets(sdims), tp_offsets(tdims)
    me = lax.axis_index("seg")
    my_t = lax.axis_index("tp")
    _, nz, nc = sdims
    my_y, my_z, my_c = me // (nz * nc), (me // nc) % nz, me % nc
    nx = tdims[1]
    my_ty, my_x = my_t // nx, my_t % nx

    def seg_to(off, sign):
        dy, dz, dc = off
        y = (my_y + dy) % sdims[0]
        z = (my_z + sign * dz + nz) % nz
        c = (my_c + dc) % nc
        return (y * nz + z) * nc + c

    def tp_to(off, sign):
        dy, dx = off
        return ((my_ty + dy) % tdims[0]) * nx + (my_x + sign * dx + nx) % nx

    barrier = pltpu.get_barrier_semaphore()
    partner = (0, 0, 1)
    for off in soffs + [partner]:
        pl.semaphore_signal(barrier, inc=1, device_id={"seg": seg_to(off, 1)})
    for off in toffs:
        pl.semaphore_signal(barrier, inc=1, device_id={"tp": tp_to(off, 1)})

    chunks_q, kq = wq.shape[0], wq.shape[1]
    chunks_c, nj = kc.shape[0], kc.shape[2]
    loads = {}
    count = [0]

    def load(name, src, dst):
        loads[name] = pltpu.make_async_copy(src, dst, dsem.at[count[0]])
        count[0] += 1
        loads[name].start()

    load("tok", tok_h, tok)
    load("owner", owner_h, owner_ref)
    load("slot", slot_h, slot_ref)
    for k in range(chunks_q):
        load(f"wq{k}", wq_h.at[pl.ds(k * kq, kq), :], wq.at[k])

    def later():
        load("wk", wk_h, wkv.at[:, pl.ds(0, DH)])
        load("wv", wv_h, wkv.at[:, pl.ds(DH, DH)])
        yield
        load("gate", gate_h, gate_ref)
        load("len", len_h, len_ref)
        load("start", start_h, start_ref)
        load("mem", mem_h, mem)
        load("norm", norm_h, norm)
        yield
        for c in range(chunks_c):
            load(f"k{c}", kc_h.at[:, pl.ds(c * nj, nj), :], kc.at[c])
            yield
        for c in range(chunks_c):
            load(f"v{c}", vc_h.at[:, pl.ds(c * nj, nj), :], vc.at[c])
            yield
        ncol = wo.shape[2]
        for k, off in enumerate(toffs + [(0, 0)]):
            column = pl.multiple_of(tp_to(off, 1) * ncol, ncol)
            load(f"wo{k}", wo_h.at[:, pl.ds(column, ncol)], wo.at[k])
            yield

    pending = later()

    loads["tok"].wait()
    acc = jnp.zeros((ROWS, GROUP * DH), F32)
    for k in range(chunks_q):
        loads[f"wq{k}"].wait()
        acc = acc + dot(tok[:, pl.ds(k * kq, kq)], wq[k])
        next(pending, None)
    query = acc.astype(BF16).astype(F32)
    qbuf[pl.ds(0, TILE), :] = stack_halves(query).astype(BF16)
    for _ in pending:
        pass

    loads["owner"].wait()
    loads["slot"].wait()
    lane = iota((1, DH), 1)
    codes = jnp.zeros((1, DH), F32)
    for r in range(ROWS):
        code = (owner_ref[r] * SLOTS + slot_ref[r] - 256).astype(F32)
        codes = jnp.where(lane % ROWS == r, code, codes)
    cbuf[0] = codes

    pl.semaphore_wait(barrier, len(soffs) + 1 + len(toffs))
    code_copies, query_copies = [], []
    for k, off in enumerate(soffs):
        target = {"seg": seg_to(off, 1)}
        copy = pltpu.make_async_remote_copy(
            cbuf.at[0], cbuf.at[k + 1], cs.at[k], cr.at[k], device_id=target
        )
        copy.start()
        code_copies.append(copy)
        copy = pltpu.make_async_remote_copy(
            qbuf.at[pl.ds(0, TILE)],
            qbuf.at[pl.ds((k + 1) * TILE, TILE)],
            qs.at[k],
            qr.at[k],
            device_id=target,
        )
        copy.start()
        query_copies.append(copy)

    loads["mem"].wait()
    loads["norm"].wait()
    flat = mem[...].reshape(SLOTS * DH, DH)
    high = flat.astype(BF16)
    mem_hi[...] = high
    mem_lo[...] = (flat - high.astype(F32)).astype(BF16)

    loads["wk"].wait()
    loads["wv"].wait()
    both = dot(tok[...], wkv[...]).astype(BF16).astype(F32)
    key_new, value_new = both[:, :DH], both[:, DH:]

    nr = GROUP * ROWS
    q32 = jnp.concatenate([query[:, h * DH : (h + 1) * DH] for h in range(GROUP)], axis=0)
    row32 = iota((nr, DH), 0) % ROWS
    scale = DH ** (-0.5)
    own = jnp.sum(q32 * jnp.concatenate([key_new] * GROUP, axis=0), axis=1, keepdims=True)
    own = own * scale

    for name in ("gate", "len", "start"):
        loads[name].wait()
    row1 = iota((nr, 1), 0) % ROWS
    first = jnp.zeros((nr, 1), jnp.int32)
    last = jnp.zeros((nr, 1), jnp.int32)
    for r in range(ROWS):
        first = jnp.where(row1 == r, start_ref[r], first)
        last = jnp.where(row1 == r, len_ref[r], last)

    rbuf[pl.ds(4 * SLOTS, DH - 4 * SLOTS), :] = jnp.zeros((DH - 4 * SLOTS, HALF), BF16)
    spread = jnp.concatenate(
        [jnp.where(row32 == r, q32, 0.0) for r in range(ROWS)], axis=1
    ).astype(BF16)
    top = own
    for c in range(chunks_c):
        loads[f"k{c}"].wait()
        keys = jnp.concatenate([kc[c, r] for r in range(ROWS)], axis=1)
        s = dot(spread, keys, ((1,), (1,))) * scale
        position = iota((nr, nj), 1) + c * nj
        s = jnp.where((position >= first) & (position < last), s, -jnp.inf)
        score[c] = s
        top = jnp.maximum(top, jnp.max(s, axis=1, keepdims=True))

    for copy in code_copies:
        copy.wait_recv()
    senders = cbuf.shape[0]
    nmsg = senders * TILE
    arrived = cbuf[...].reshape(senders, DH).astype(BF16)
    which = (iota((nmsg, senders), 0) // TILE == iota((nmsg, senders), 1)).astype(F32)
    spread_codes = dot(which.astype(BF16), arrived)
    mrow, mlane = iota((nmsg, DH), 0) % TILE, iota((nmsg, DH), 1)
    code_col = jnp.sum(jnp.where(mrow == mlane, spread_codes, 0.0), axis=1, keepdims=True)
    holder = jnp.where(mlane < 2 * SLOTS, me, seg_to(partner, 1))
    wanted = (holder * SLOTS - 256 + mlane % SLOTS).astype(F32)
    hit = (code_col == wanted) & ((mlane // SLOTS) % 2 == mrow // ROWS) & (mlane < 4 * SLOTS)
    picks = jnp.where(hit, 1.0, 0.0)
    sel_t[...] = picks.astype(BF16)
    sel[...] = picks.T[: 4 * SLOTS].astype(BF16)

    own_weight = jnp.exp(own - top)
    total = own_weight
    for c in range(chunks_c):
        w = jnp.exp(score[c] - top)
        score[c] = w
        total = total + jnp.sum(w, axis=1, keepdims=True)
    share = 1.0 / total
    own_prob = (own_weight * share).astype(BF16).astype(F32)

    for copy in query_copies:
        copy.wait_recv()
    picked = dot(sel[...], qbuf[...])
    own_half, other_half = pl.ds(0, 2 * SLOTS), pl.ds(2 * SLOTS, 2 * SLOTS)
    xbuf[own_half, :] = picked[2 * SLOTS :].astype(BF16)
    other = {"seg": seg_to(partner, 1)}
    pick_copy = pltpu.make_async_remote_copy(
        xbuf.at[own_half], xbuf.at[other_half], ps.at[0], pr.at[0], device_id=other
    )
    pick_copy.start()
    pick_copy.wait_recv()
    picked = picked[: 2 * SLOTS] + xbuf[other_half, :].astype(F32)
    lifted = stack_heads(picked, SLOTS)
    lifted = jnp.where(lifted > 0, lifted + 1.0, jnp.exp(jnp.minimum(lifted, 0.0)))
    norms = jnp.concatenate([norm[...]] * GROUP, axis=0)
    denominator = jnp.sum(lifted * norms, axis=1, keepdims=True)
    nl = GROUP * SLOTS
    slot_row = iota((nl, DH), 0) % SLOTS
    part_hi = lifted.astype(BF16).astype(F32)
    part_lo = lifted - part_hi
    wide_hi = jnp.concatenate(
        [jnp.where(slot_row == t, part_hi, 0.0) for t in range(SLOTS)], axis=1
    ).astype(BF16)
    wide_lo = jnp.concatenate(
        [jnp.where(slot_row == t, part_lo, 0.0) for t in range(SLOTS)], axis=1
    ).astype(BF16)
    stacked = dot(jnp.concatenate([wide_hi, wide_lo], axis=0), mem_hi[...])
    numerator = stacked[:nl] + stacked[nl:] + dot(wide_hi, mem_lo[...])
    read = numerator / denominator
    parts = [read[h * SLOTS : (h + 1) * SLOTS] for h in range(GROUP)]
    rbuf[own_half, :] = jnp.concatenate(
        [jnp.concatenate(parts[:2], axis=1), jnp.concatenate(parts[2:], axis=1)], axis=0
    ).astype(BF16)
    swap_copy = pltpu.make_async_remote_copy(
        rbuf.at[own_half], rbuf.at[other_half], ps.at[1], pr.at[1], device_id=other
    )
    swap_copy.start()
    swap_copy.wait_recv()
    rsend[...] = dot(sel_t[...], rbuf[...]).astype(BF16)
    read_copies = []
    for k, off in enumerate(soffs):
        copy = pltpu.make_async_remote_copy(
            rsend.at[pl.ds((k + 1) * TILE, TILE)],
            rrecv.at[pl.ds(k * TILE, TILE)],
            rs.at[k],
            rr.at[k],
            device_id={"seg": seg_to(off, -1)},
        )
        copy.start()
        read_copies.append(copy)

    wide = jnp.zeros((nr, ROWS * DH), F32)
    for c in range(chunks_c):
        loads[f"v{c}"].wait()
        values = jnp.concatenate([vc[c, r] for r in range(ROWS)], axis=1)
        wide = wide + dot((score[c] * share).astype(BF16), values)
    local = own_prob * jnp.concatenate([value_new] * GROUP, axis=0)
    for r in range(ROWS):
        local = local + jnp.where(row32 == r, wide[:, r * DH : (r + 1) * DH], 0.0)
    gates = jax.nn.sigmoid(
        jnp.concatenate([jnp.full((ROWS, DH), gate_ref[h], F32) for h in range(GROUP)], axis=0)
    )
    local = (1.0 - gates) * local
    for k in range(tp_count):
        loads[f"wo{k}"].wait()

    for copy in read_copies:
        copy.wait_recv()
    back = rsend[pl.ds(0, TILE), :].astype(F32)
    for k in range(len(soffs)):
        back = back + rrecv[pl.ds(k * TILE, TILE), :].astype(F32)
    mixed = gates * stack_heads(back, ROWS) + local
    attended = jnp.concatenate(
        [mixed[h * ROWS : (h + 1) * ROWS] for h in range(GROUP)], axis=1
    ).astype(BF16)

    out_copies = []
    for k, off in enumerate(toffs):
        tsend[k] = stack_halves(dot(attended, wo[k])).astype(BF16)
        copy = pltpu.make_async_remote_copy(
            tsend.at[k], trecv.at[k], ts.at[k], tr.at[k], device_id={"tp": tp_to(off, 1)}
        )
        copy.start()
        out_copies.append(copy)
    result = stack_halves(dot(attended, wo[tp_count - 1]))
    for k, copy in enumerate(out_copies):
        copy.wait_recv()
    for k in range(len(toffs)):
        result = result + trecv[k].astype(F32)
    out_ref[...] = jnp.concatenate([result[:ROWS], result[ROWS:]], axis=1).astype(BF16)
    for copy in code_copies + query_copies + read_copies + out_copies + [pick_copy, swap_copy]:
        copy.wait_send()


def body(
    tokens,
    w_query,
    w_key,
    w_value,
    w_out,
    gate_bias,
    mem_store,
    norm_store,
    k_cache,
    v_cache,
    home_owner,
    home_slot,
    cache_len,
    win_start,
):
    seg_count, tp_count = lax.axis_size("seg"), lax.axis_size("tp")
    depth = tokens.shape[1]
    window = k_cache.shape[1]
    width = w_query.shape[1]
    chunks_q, chunks_c = 8, 4
    nj = window // chunks_c
    columns = w_out.shape[1] // tp_count
    senders = seg_count // seg_dims(seg_count)[2]
    peers, partners = senders - 1, tp_count - 1
    nmsg = senders * TILE
    anywhere = pl.BlockSpec(memory_space=pl.ANY)
    dma = pltpu.SemaphoreType.DMA
    loads = 1 + chunks_q + 9 + 2 * chunks_c + tp_count
    return pl.pallas_call(
        functools.partial(kernel, seg_count, tp_count),
        out_shape=pltpu.VMEM((ROWS, columns), BF16),
        in_specs=[anywhere] * 14,
        out_specs=pl.BlockSpec(memory_space=pltpu.VMEM),
        scratch_shapes=[
            pltpu.SMEM((GROUP,), F32),
            pltpu.SMEM((ROWS,), jnp.int32),
            pltpu.SMEM((ROWS,), jnp.int32),
            pltpu.SMEM((ROWS,), jnp.int32),
            pltpu.SMEM((ROWS,), jnp.int32),
            pltpu.VMEM((ROWS, depth), BF16),
            pltpu.VMEM((chunks_q, depth // chunks_q, width), BF16),
            pltpu.VMEM((depth, 2 * DH), BF16),
            pltpu.VMEM((tp_count, width, columns), BF16),
            pltpu.VMEM((SLOTS, DH, DH), F32),
            pltpu.VMEM((SLOTS, DH), F32),
            pltpu.VMEM((chunks_c, ROWS, nj, DH), BF16),
            pltpu.VMEM((chunks_c, ROWS, nj, DH), BF16),
            pltpu.VMEM((SLOTS * DH, DH), BF16),
            pltpu.VMEM((SLOTS * DH, DH), BF16),
            pltpu.VMEM((nmsg, HALF), BF16),
            pltpu.VMEM((senders, 1, DH), F32),
            pltpu.VMEM((4 * SLOTS, nmsg), BF16),
            pltpu.VMEM((nmsg, DH), BF16),
            pltpu.VMEM((4 * SLOTS, HALF), BF16),
            pltpu.VMEM((DH, HALF), BF16),
            pltpu.VMEM((nmsg, HALF), BF16),
            pltpu.VMEM((peers * TILE, HALF), BF16),
            pltpu.VMEM((partners, 2 * ROWS, columns // 2), BF16),
            pltpu.VMEM((partners, 2 * ROWS, columns // 2), BF16),
            pltpu.VMEM((chunks_c, GROUP * ROWS, nj), F32),
            dma((loads,)),
            dma((peers,)),
            dma((peers,)),
            dma((peers,)),
            dma((peers,)),
            dma((peers,)),
            dma((peers,)),
            dma((partners,)),
            dma((partners,)),
            dma((2,)),
            dma((2,)),
        ],
        compiler_params=pltpu.CompilerParams(
            collective_id=0, has_side_effects=True, vmem_limit_bytes=60 * 1024 * 1024
        ),
    )(
        gate_bias,
        home_owner,
        home_slot,
        cache_len,
        win_start,
        tokens,
        w_query,
        w_key,
        w_value,
        w_out,
        mem_store.reshape(SLOTS, DH, DH),
        norm_store.reshape(SLOTS, DH),
        k_cache,
        v_cache,
    )


def solution(mesh):
    placed = (
        P("seg", None),
        P(None, "tp"),
        P(None, "tp"),
        P(None, "tp"),
        P("tp", None),
        P("tp"),
        P("seg", "tp", None, None),
        P("seg", "tp", None),
        P("seg", None, "tp"),
        P("seg", None, "tp"),
        P("seg"),
        P("seg"),
        P("seg"),
        P("seg"),
    )
    return jax.shard_map(
        body, mesh=mesh, in_specs=placed, out_specs=P("seg", "tp"), check_vma=False
    )
```

```python
import functools

import jax
import jax.numpy as jnp
from jax import lax
from jax.experimental import pallas as pl
from jax.experimental.pallas import tpu as pltpu
from jax.sharding import PartitionSpec as P

DH = 128
GROUP = 4
ROWS = 8
SLOTS = 16
HALF = 2 * DH
TILE = 2 * ROWS

F32 = jnp.float32
BF16 = jnp.bfloat16


def seg_dims(count):
    return {32: (2, 8, 2), 8: (2, 2, 2)}[count]


def tp_dims(count):
    return {8: (2, 4), 2: (2, 1)}[count]


def seg_offsets(dims):
    ny, nz, _ = dims
    found = []
    for dy in range(ny):
        for dz in range(nz):
            if (dy, dz) != (0, 0):
                found.append((-(6 * dy + min(dz, nz - dz)), dy, dz))
    found.sort()
    return [(dy, dz, 0) for _, dy, dz in found]


def tp_offsets(dims):
    ny, nx = dims
    found = []
    for dy in range(ny):
        for dx in range(nx):
            if (dy, dx) != (0, 0):
                found.append((-(dy + min(dx, nx - dx)), dy, dx))
    found.sort()
    return [(dy, dx) for _, dy, dx in found]


def iota(shape, dim):
    return lax.broadcasted_iota(jnp.int32, shape, dim)


def dot(a, b, dims=((1,), (0,))):
    return lax.dot_general(a, b, (dims, ((), ())), preferred_element_type=F32)


def stack_heads(x, rows):
    return jnp.concatenate(
        [x[:rows, :DH], x[:rows, DH:], x[rows:, :DH], x[rows:, DH:]], axis=0
    )


def stack_halves(x):
    half = x.shape[1] // 2
    return jnp.concatenate([x[:, :half], x[:, half:]], axis=0)


def kernel(
    seg_count,
    tp_count,
    gate_h,
    owner_h,
    slot_h,
    len_h,
    start_h,
    tok_h,
    wq_h,
    wk_h,
    wv_h,
    wo_h,
    mem_h,
    norm_h,
    kc_h,
    vc_h,
    out_ref,
    gate_ref,
    owner_ref,
    slot_ref,
    len_ref,
    start_ref,
    tok,
    wq,
    wkv,
    wo,
    mem,
    norm,
    kc,
    vc,
    mem_hi,
    mem_lo,
    qbuf,
    cbuf,
    sel,
    sel_t,
    xbuf,
    rbuf,
    rsend,
    rrecv,
    tsend,
    trecv,
    score,
    dsem,
    qs,
    qr,
    cs,
    cr,
    rs,
    rr,
    ts,
    tr,
    ps,
    pr,
):
    sdims, tdims = seg_dims(seg_count), tp_dims(tp_count)
    soffs, toffs = seg_offsets(sdims), tp_offsets(tdims)
    me = lax.axis_index("seg")
    my_t = lax.axis_index("tp")
    _, nz, nc = sdims
    my_y, my_z, my_c = me // (nz * nc), (me // nc) % nz, me % nc
    nx = tdims[1]
    my_ty, my_x = my_t // nx, my_t % nx

    def seg_to(off, sign):
        dy, dz, dc = off
        y = (my_y + dy) % sdims[0]
        z = (my_z + sign * dz + nz) % nz
        c = (my_c + dc) % nc
        return (y * nz + z) * nc + c

    def tp_to(off, sign):
        dy, dx = off
        return ((my_ty + dy) % tdims[0]) * nx + (my_x + sign * dx + nx) % nx

    barrier = pltpu.get_barrier_semaphore()
    partner = (0, 0, 1)
    for off in soffs + [partner]:
        pl.semaphore_signal(barrier, inc=1, device_id={"seg": seg_to(off, 1)})
    for off in toffs:
        pl.semaphore_signal(barrier, inc=1, device_id={"tp": tp_to(off, 1)})

    chunks_q, kq = wq.shape[0], wq.shape[1]
    chunks_c, nj = kc.shape[0], kc.shape[2]
    loads = {}
    count = [0]

    def load(name, src, dst):
        loads[name] = pltpu.make_async_copy(src, dst, dsem.at[count[0]])
        count[0] += 1
        loads[name].start()

    load("tok", tok_h, tok)
    load("owner", owner_h, owner_ref)
    load("slot", slot_h, slot_ref)
    for k in range(chunks_q):
        load(f"wq{k}", wq_h.at[pl.ds(k * kq, kq), :], wq.at[k])

    def later():
        load("wk", wk_h, wkv.at[:, pl.ds(0, DH)])
        load("wv", wv_h, wkv.at[:, pl.ds(DH, DH)])
        yield
        load("gate", gate_h, gate_ref)
        load("len", len_h, len_ref)
        load("start", start_h, start_ref)
        load("mem", mem_h, mem)
        load("norm", norm_h, norm)
        yield
        for c in range(chunks_c):
            load(f"k{c}", kc_h.at[:, pl.ds(c * nj, nj), :], kc.at[c])
            yield
        for c in range(chunks_c):
            load(f"v{c}", vc_h.at[:, pl.ds(c * nj, nj), :], vc.at[c])
            yield
        ncol = wo.shape[2]
        for k, off in enumerate(toffs + [(0, 0)]):
            column = pl.multiple_of(tp_to(off, 1) * ncol, ncol)
            load(f"wo{k}", wo_h.at[:, pl.ds(column, ncol)], wo.at[k])
            yield

    pending = later()

    loads["tok"].wait()
    acc = jnp.zeros((ROWS, GROUP * DH), F32)
    for k in range(chunks_q):
        loads[f"wq{k}"].wait()
        acc = acc + dot(tok[:, pl.ds(k * kq, kq)], wq[k])
        next(pending, None)
    query = acc.astype(BF16).astype(F32)
    qbuf[pl.ds(0, TILE), :] = stack_halves(query).astype(BF16)
    for _ in pending:
        pass

    loads["owner"].wait()
    loads["slot"].wait()
    lane = iota((1, DH), 1)
    codes = jnp.zeros((1, DH), F32)
    for r in range(ROWS):
        code = (owner_ref[r] * SLOTS + slot_ref[r] - 256).astype(F32)
        codes = jnp.where(lane % ROWS == r, code, codes)
    cbuf[0] = codes

    pl.semaphore_wait(barrier, len(soffs) + 1 + len(toffs))
    code_copies, query_copies = [], []
    for k, off in enumerate(soffs):
        target = {"seg": seg_to(off, 1)}
        copy = pltpu.make_async_remote_copy(
            cbuf.at[0], cbuf.at[k + 1], cs.at[k], cr.at[k], device_id=target
        )
        copy.start()
        code_copies.append(copy)
        copy = pltpu.make_async_remote_copy(
            qbuf.at[pl.ds(0, TILE)],
            qbuf.at[pl.ds((k + 1) * TILE, TILE)],
            qs.at[k],
            qr.at[k],
            device_id=target,
        )
        copy.start()
        query_copies.append(copy)

    loads["mem"].wait()
    loads["norm"].wait()
    flat = mem[...].reshape(SLOTS * DH, DH)
    high = flat.astype(BF16)
    mem_hi[...] = high
    mem_lo[...] = (flat - high.astype(F32)).astype(BF16)

    loads["wk"].wait()
    loads["wv"].wait()
    both = dot(tok[...], wkv[...]).astype(BF16).astype(F32)
    key_new, value_new = both[:, :DH], both[:, DH:]

    nr = GROUP * ROWS
    q32 = jnp.concatenate([query[:, h * DH : (h + 1) * DH] for h in range(GROUP)], axis=0)
    row32 = iota((nr, DH), 0) % ROWS
    scale = DH ** (-0.5)
    own = jnp.sum(q32 * jnp.concatenate([key_new] * GROUP, axis=0), axis=1, keepdims=True)
    own = own * scale

    for name in ("gate", "len", "start"):
        loads[name].wait()
    row1 = iota((nr, 1), 0) % ROWS
    first = jnp.zeros((nr, 1), jnp.int32)
    last = jnp.zeros((nr, 1), jnp.int32)
    for r in range(ROWS):
        first = jnp.where(row1 == r, start_ref[r], first)
        last = jnp.where(row1 == r, len_ref[r], last)

    rbuf[pl.ds(4 * SLOTS, DH - 4 * SLOTS), :] = jnp.zeros((DH - 4 * SLOTS, HALF), BF16)
    spread = jnp.concatenate(
        [jnp.where(row32 == r, q32, 0.0) for r in range(ROWS)], axis=1
    ).astype(BF16)
    top = own
    for c in range(chunks_c):
        loads[f"k{c}"].wait()
        keys = jnp.concatenate([kc[c, r] for r in range(ROWS)], axis=1)
        s = dot(spread, keys, ((1,), (1,))) * scale
        position = iota((nr, nj), 1) + c * nj
        s = jnp.where((position >= first) & (position < last), s, -jnp.inf)
        score[c] = s
        top = jnp.maximum(top, jnp.max(s, axis=1, keepdims=True))

    for copy in code_copies:
        copy.wait_recv()
    senders = cbuf.shape[0]
    nmsg = senders * TILE
    arrived = cbuf[...].reshape(senders, DH).astype(BF16)
    which = (iota((nmsg, senders), 0) // TILE == iota((nmsg, senders), 1)).astype(F32)
    spread_codes = dot(which.astype(BF16), arrived)
    mrow, mlane = iota((nmsg, DH), 0) % TILE, iota((nmsg, DH), 1)
    code_col = jnp.sum(jnp.where(mrow == mlane, spread_codes, 0.0), axis=1, keepdims=True)
    holder = jnp.where(mlane < 2 * SLOTS, me, seg_to(partner, 1))
    wanted = (holder * SLOTS - 256 + mlane % SLOTS).astype(F32)
    hit = (code_col == wanted) & ((mlane // SLOTS) % 2 == mrow // ROWS) & (mlane < 4 * SLOTS)
    picks = jnp.where(hit, 1.0, 0.0)
    sel_t[...] = picks.astype(BF16)
    sel[...] = picks.T[: 4 * SLOTS].astype(BF16)

    own_weight = jnp.exp(own - top)
    total = own_weight
    for c in range(chunks_c):
        w = jnp.exp(score[c] - top)
        score[c] = w
        total = total + jnp.sum(w, axis=1, keepdims=True)
    share = 1.0 / total
    own_prob = (own_weight * share).astype(BF16).astype(F32)

    for copy in query_copies:
        copy.wait_recv()
    picked = dot(sel[...], qbuf[...])
    own_half, other_half = pl.ds(0, 2 * SLOTS), pl.ds(2 * SLOTS, 2 * SLOTS)
    xbuf[own_half, :] = picked[2 * SLOTS :].astype(BF16)
    other = {"seg": seg_to(partner, 1)}
    pick_copy = pltpu.make_async_remote_copy(
        xbuf.at[own_half], xbuf.at[other_half], ps.at[0], pr.at[0], device_id=other
    )
    pick_copy.start()
    pick_copy.wait_recv()
    picked = picked[: 2 * SLOTS] + xbuf[other_half, :].astype(F32)
    lifted = stack_heads(picked, SLOTS)
    lifted = jnp.where(lifted > 0, lifted + 1.0, jnp.exp(jnp.minimum(lifted, 0.0)))
    norms = jnp.concatenate([norm[...]] * GROUP, axis=0)
    denominator = jnp.sum(lifted * norms, axis=1, keepdims=True)
    nl = GROUP * SLOTS
    slot_row = iota((nl, DH), 0) % SLOTS
    part_hi = lifted.astype(BF16).astype(F32)
    part_lo = lifted - part_hi
    wide_hi = jnp.concatenate(
        [jnp.where(slot_row == t, part_hi, 0.0) for t in range(SLOTS)], axis=1
    ).astype(BF16)
    wide_lo = jnp.concatenate(
        [jnp.where(slot_row == t, part_lo, 0.0) for t in range(SLOTS)], axis=1
    ).astype(BF16)
    stacked = dot(jnp.concatenate([wide_hi, wide_lo], axis=0), mem_hi[...])
    numerator = stacked[:nl] + stacked[nl:] + dot(wide_hi, mem_lo[...])
    read = numerator / denominator
    parts = [read[h * SLOTS : (h + 1) * SLOTS] for h in range(GROUP)]
    rbuf[own_half, :] = jnp.concatenate(
        [jnp.concatenate(parts[:2], axis=1), jnp.concatenate(parts[2:], axis=1)], axis=0
    ).astype(BF16)
    swap_copy = pltpu.make_async_remote_copy(
        rbuf.at[own_half], rbuf.at[other_half], ps.at[1], pr.at[1], device_id=other
    )
    swap_copy.start()
    swap_copy.wait_recv()
    half_rows = rsend.shape[0] // 2
    read_copies = []
    for part in range(2):
        block = pl.ds(part * half_rows, half_rows)
        rsend[block, :] = dot(sel_t[block, :], rbuf[...]).astype(BF16)
        per_half = half_rows // TILE
        for tile in range(max(1, part * per_half), (part + 1) * per_half):
            k = tile - 1
            copy = pltpu.make_async_remote_copy(
                rsend.at[pl.ds(tile * TILE, TILE)],
                rrecv.at[pl.ds(k * TILE, TILE)],
                rs.at[k],
                rr.at[k],
                device_id={"seg": seg_to(soffs[k], -1)},
            )
            copy.start()
            read_copies.append(copy)

    wide = jnp.zeros((nr, ROWS * DH), F32)
    for c in range(chunks_c):
        loads[f"v{c}"].wait()
        values = jnp.concatenate([vc[c, r] for r in range(ROWS)], axis=1)
        wide = wide + dot((score[c] * share).astype(BF16), values)
    local = own_prob * jnp.concatenate([value_new] * GROUP, axis=0)
    for r in range(ROWS):
        local = local + jnp.where(row32 == r, wide[:, r * DH : (r + 1) * DH], 0.0)
    gates = jax.nn.sigmoid(
        jnp.concatenate([jnp.full((ROWS, DH), gate_ref[h], F32) for h in range(GROUP)], axis=0)
    )
    local = (1.0 - gates) * local
    for k in range(tp_count):
        loads[f"wo{k}"].wait()

    for copy in read_copies:
        copy.wait_recv()
    back = rsend[pl.ds(0, TILE), :].astype(F32)
    for k in range(len(soffs)):
        back = back + rrecv[pl.ds(k * TILE, TILE), :].astype(F32)
    mixed = gates * stack_heads(back, ROWS) + local
    attended = jnp.concatenate(
        [mixed[h * ROWS : (h + 1) * ROWS] for h in range(GROUP)], axis=1
    ).astype(BF16)

    out_copies = []
    for k, off in enumerate(toffs):
        tsend[k] = stack_halves(dot(attended, wo[k])).astype(BF16)
        copy = pltpu.make_async_remote_copy(
            tsend.at[k], trecv.at[k], ts.at[k], tr.at[k], device_id={"tp": tp_to(off, 1)}
        )
        copy.start()
        out_copies.append(copy)
    result = stack_halves(dot(attended, wo[tp_count - 1]))
    for k, copy in enumerate(out_copies):
        copy.wait_recv()
    for k in range(len(toffs)):
        result = result + trecv[k].astype(F32)
    out_ref[...] = jnp.concatenate([result[:ROWS], result[ROWS:]], axis=1).astype(BF16)
    for copy in code_copies + query_copies + read_copies + out_copies + [pick_copy, swap_copy]:
        copy.wait_send()


def body(
    tokens,
    w_query,
    w_key,
    w_value,
    w_out,
    gate_bias,
    mem_store,
    norm_store,
    k_cache,
    v_cache,
    home_owner,
    home_slot,
    cache_len,
    win_start,
):
    seg_count, tp_count = lax.axis_size("seg"), lax.axis_size("tp")
    depth = tokens.shape[1]
    window = k_cache.shape[1]
    width = w_query.shape[1]
    chunks_q, chunks_c = 8, 4
    nj = window // chunks_c
    columns = w_out.shape[1] // tp_count
    senders = seg_count // seg_dims(seg_count)[2]
    peers, partners = senders - 1, tp_count - 1
    nmsg = senders * TILE
    anywhere = pl.BlockSpec(memory_space=pl.ANY)
    dma = pltpu.SemaphoreType.DMA
    loads = 1 + chunks_q + 9 + 2 * chunks_c + tp_count
    return pl.pallas_call(
        functools.partial(kernel, seg_count, tp_count),
        out_shape=pltpu.VMEM((ROWS, columns), BF16),
        in_specs=[anywhere] * 14,
        out_specs=pl.BlockSpec(memory_space=pltpu.VMEM),
        scratch_shapes=[
            pltpu.SMEM((GROUP,), F32),
            pltpu.SMEM((ROWS,), jnp.int32),
            pltpu.SMEM((ROWS,), jnp.int32),
            pltpu.SMEM((ROWS,), jnp.int32),
            pltpu.SMEM((ROWS,), jnp.int32),
            pltpu.VMEM((ROWS, depth), BF16),
            pltpu.VMEM((chunks_q, depth // chunks_q, width), BF16),
            pltpu.VMEM((depth, 2 * DH), BF16),
            pltpu.VMEM((tp_count, width, columns), BF16),
            pltpu.VMEM((SLOTS, DH, DH), F32),
            pltpu.VMEM((SLOTS, DH), F32),
            pltpu.VMEM((chunks_c, ROWS, nj, DH), BF16),
            pltpu.VMEM((chunks_c, ROWS, nj, DH), BF16),
            pltpu.VMEM((SLOTS * DH, DH), BF16),
            pltpu.VMEM((SLOTS * DH, DH), BF16),
            pltpu.VMEM((nmsg, HALF), BF16),
            pltpu.VMEM((senders, 1, DH), F32),
            pltpu.VMEM((4 * SLOTS, nmsg), BF16),
            pltpu.VMEM((nmsg, DH), BF16),
            pltpu.VMEM((4 * SLOTS, HALF), BF16),
            pltpu.VMEM((DH, HALF), BF16),
            pltpu.VMEM((nmsg, HALF), BF16),
            pltpu.VMEM((peers * TILE, HALF), BF16),
            pltpu.VMEM((partners, 2 * ROWS, columns // 2), BF16),
            pltpu.VMEM((partners, 2 * ROWS, columns // 2), BF16),
            pltpu.VMEM((chunks_c, GROUP * ROWS, nj), F32),
            dma((loads,)),
            dma((peers,)),
            dma((peers,)),
            dma((peers,)),
            dma((peers,)),
            dma((peers,)),
            dma((peers,)),
            dma((partners,)),
            dma((partners,)),
            dma((2,)),
            dma((2,)),
        ],
        compiler_params=pltpu.CompilerParams(
            collective_id=0, has_side_effects=True, vmem_limit_bytes=60 * 1024 * 1024
        ),
    )(
        gate_bias,
        home_owner,
        home_slot,
        cache_len,
        win_start,
        tokens,
        w_query,
        w_key,
        w_value,
        w_out,
        mem_store.reshape(SLOTS, DH, DH),
        norm_store.reshape(SLOTS, DH),
        k_cache,
        v_cache,
    )


def solution(mesh):
    placed = (
        P("seg", None),
        P(None, "tp"),
        P(None, "tp"),
        P(None, "tp"),
        P("tp", None),
        P("tp"),
        P("seg", "tp", None, None),
        P("seg", "tp", None),
        P("seg", None, "tp"),
        P("seg", None, "tp"),
        P("seg"),
        P("seg"),
        P("seg"),
        P("seg"),
    )
    return jax.shard_map(
        body, mesh=mesh, in_specs=placed, out_specs=P("seg", "tp"), check_vma=False
    )
```
